32 devices in a mesh: dp: 8 (over y, x, core), mp: 4 (over z).
Axes of the slice: x: 2, y: 2, z: 4, core: 2. Of those that a mesh axis runs over, the one named last changes fastest.
Arguments:
- hidden_rows: bfloat16 [4096, 3584], P('dp'), may hold values from -6 to 6
- key_grad: bfloat16 [4096, 512], P('dp', 'mp'), may hold values from -6 to 6
- value_grad: bfloat16 [4096, 512], P('dp', 'mp'), may hold values from -6 to 6
- visual_rows: bfloat16 [2048, 1024], P('dp'), may hold values from -6 to 6
- visual_cotangent: bfloat16 [8, 4, 64, 3584], P('dp'), may hold values from -6 to 6
- norm_gain: float32 [1024], replicated, may hold values from 0.25 to 1.75
- norm_bias: float32 [1024], replicated, may hold values from -3 to 3
- fc1_weight: bfloat16 [1024, 4096], P(None, 'mp'), may hold values from -0.1875 to 0.1875
- fc1_bias: float32 [4096], P('mp'), may hold values from -3 to 3
- fc2_weight: bfloat16 [4096, 1024], P('mp'), may hold values from -0.09375 to 0.09375
- fc2_bias: float32 [1024], replicated, may hold values from -3 to 3
- layer_scale: float32 [1024], replicated, may hold values from 0.3 to 1.5
- token_counts: int32 [8, 8], P('dp'), may hold values from 1 to 32, as said below
- dest_offsets: int32 [8, 8], P('dp'), may hold values from 1 to 4, as said below
Outputs:
- key_weight_grad: float32 [3592, 512], P('dp', 'mp')
- value_weight_grad: float32 [3592, 512], P('dp', 'mp')
- projector_grad: float32 [3592, 1024], P('dp', 'mp')
- handoff: bfloat16 [8, 4, 64, 1024], P('dp', None, None, 'mp')
The draws below stay inside these ranges and needn't reach their ends.
Inputs may be any that keep to these rules, and one draw needn't show every extreme that they name: `token_counts`: on every data rank the images of one distance, chosen per rank, all have 32 rows. `dest_offsets`: every data rank sends exactly 2 images to each distance from 1 to 4.
All inputs are finite; a program needn't handle non-finite values.
Results may differ from the reference program's by a relative error of at most 0.0046.
Values may be sent and summed in bfloat16 or wider, within the bound.
A program may use at most 64 MiB of HBM per device.

```python
import math
import jax
import jax.numpy as jnp
from jax import lax

D = 3584
KV_WIDTH = 512
FEAT = 1024
MLP = 4096
TOK_DEV = 512
MOST_TOK = 32
SPREAD = 4
IMG_DEV = 8
ROWS_DEV = 256
CAP = 64
TOKENS = 4096
D_PAD = 3592
N_DP = 8


def routing_table(key):
    base = jax.random.fold_in(key, 11)
    source_keys = jax.random.split(base, N_DP)

    def one_source(source_key):
        first, second, third = jax.random.split(source_key, 3)
        order = jax.random.permutation(first, IMG_DEV)
        offsets = (order % SPREAD + 1).astype(jnp.int32)
        counts = jax.random.randint(second, (IMG_DEV,), 1, MOST_TOK + 1).astype(jnp.int32)
        filled = jax.random.randint(third, (), 1, SPREAD + 1).astype(jnp.int32)
        counts = jnp.where(offsets == filled, MOST_TOK, counts).astype(jnp.int32)
        return (counts, offsets)
    return jax.vmap(one_source)(source_keys)


def draw_token_counts(key, part):
    return routing_table(key)[0]


def draw_dest_offsets(key, part):
    return routing_table(key)[1]


def strengthened(values, own_key, source, target, shards_of, factor):
    owner, partner = [(jnp.arange(values.shape[dim]) // (values.shape[dim] // shards_of)).reshape([-1 if axis == dim else 1 for axis in range(values.ndim)]) for dim in (source, target)]
    chosen = jax.random.permutation(own_key, shards_of)[partner]
    strong = (owner == chosen) | (owner == (partner + shards_of // 2) % shards_of)
    return jnp.where(strong, factor * values, values)


def block_levels(key, shape, shards, smallest, high):
    loudness = 1.0
    for dim, blocks in shards:
        draws = jax.random.uniform(jax.random.fold_in(jax.random.fold_in(key, 6), dim), (blocks,), jnp.float32, smallest / len(shards), high / len(shards))
        loudness = loudness * jnp.repeat(jnp.exp(draws), shape[dim] // blocks).reshape((-1,) + (1,) * (len(shape) - 1 - dim))
    return loudness


def noise(own_key, shape, scale, reach, cuts=(), dtype=jnp.bfloat16):
    result = scale * jax.random.normal(own_key, shape, jnp.float32)
    if cuts:
        result = result * block_levels(own_key, shape, cuts, -0.22, 0.18)
    return jnp.clip(result, -reach, reach).astype(dtype)


def noise_with(stream_key, shape, spread, bound, cuts, heavy, dtype=jnp.bfloat16):
    entries = spread * jax.random.normal(stream_key, shape, jnp.float32)
    if cuts:
        entries = entries * block_levels(stream_key, shape, cuts, -0.22, 0.18)
    return jnp.clip(strengthened(entries, jax.random.fold_in(stream_key, 3), *heavy), -bound, bound).astype(dtype)


def setup_inputs(seed: int = 0) -> dict:
    keys = jax.random.split(jax.random.key(seed), 15)
    return {
        "hidden_rows": noise_with(keys[0], (TOKENS, D), 1.0, 6.0, ((0, 8),), (0, 1, 8, 2.0)),
        "key_grad": noise(keys[1], (TOKENS, KV_WIDTH), 1.0, 6.0, ((0, 8), (1, 4))),
        "value_grad": noise(keys[2], (TOKENS, KV_WIDTH), 1.0, 6.0, ((0, 8), (1, 4))),
        "visual_rows": noise(keys[3], (N_DP * ROWS_DEV, FEAT), 1.0, 6.0, ((0, 8),)),
        "visual_cotangent": noise_with(keys[4], (N_DP, SPREAD, CAP, D), 1.0, 6.0, ((0, 8),), (0, 3, 8, 2.0)),
        "norm_gain": jnp.clip(1.0 + 0.15 * jax.random.normal(keys[5], (FEAT,), jnp.float32), 0.25, 1.75),
        "norm_bias": noise(keys[6], (FEAT,), 0.5, 3.0, (), jnp.float32),
        "fc1_weight": noise(keys[7], (FEAT, MLP), FEAT ** -0.5, 0.1875, ((1, 4),)),
        "fc1_bias": noise(keys[8], (MLP,), 0.5, 3.0, ((0, 4),), jnp.float32),
        "fc2_weight": noise(keys[9], (MLP, FEAT), MLP ** -0.5, 0.09375, ((0, 4),)),
        "fc2_bias": noise(keys[10], (FEAT,), 0.5, 3.0, (), jnp.float32),
        "layer_scale": jnp.clip(jnp.exp(jax.random.uniform(keys[11], (FEAT,), jnp.float32, math.log(0.3), math.log(1.5))), 0.3, 1.5),
        "token_counts": draw_token_counts(jax.random.fold_in(keys[14], 71), 0),
        "dest_offsets": draw_dest_offsets(jax.random.fold_in(keys[14], 71), 0),
    }


def pack_rows(rows, counts, offsets):
    total_rows = rows.shape[0]
    images = counts.shape[0]
    counts = counts.astype(jnp.int32)
    offsets = offsets.astype(jnp.int32)
    ends = jnp.cumsum(counts).astype(jnp.int32)
    starts = (ends - counts).astype(jnp.int32)
    places = jnp.arange(total_rows).astype(jnp.int32)
    image_ids = jnp.arange(images).astype(jnp.int32)
    owner = lax.optimization_barrier(jnp.sum((places[:, None] >= ends[None, :]).astype(jnp.int32), axis=1)).astype(jnp.int32)
    member = (owner[:, None] == image_ids[None, :]).astype(jnp.int32)
    earlier = (image_ids[None, :] < image_ids[:, None]) & (offsets[None, :] == offsets[:, None])
    before = lax.optimization_barrier(jnp.sum(earlier.astype(jnp.int32) * counts[None, :], axis=1)).astype(jnp.int32)
    row_dest = lax.optimization_barrier(jnp.sum(member * offsets[None, :], axis=1)).astype(jnp.int32)
    row_start = lax.optimization_barrier(jnp.sum(member * starts[None, :], axis=1)).astype(jnp.int32)
    row_before = lax.optimization_barrier(jnp.sum(member * before[None, :], axis=1)).astype(jnp.int32)
    slot_index = row_before + places - row_start
    target = jnp.where(places < ends[images - 1], (row_dest - 1) * CAP + slot_index, -1).astype(jnp.int32)
    slot_ids = jnp.arange(SPREAD * CAP).astype(jnp.int32)
    select = (slot_ids[:, None] == target[None, :]).astype(jnp.bfloat16)
    packed = jnp.dot(select, rows, preferred_element_type=jnp.float32).astype(jnp.bfloat16)
    return packed.reshape(SPREAD, CAP, rows.shape[1])

def encode(rows, norm_gain, norm_bias, fc1_weight, fc1_bias, fc2_weight, fc2_bias, layer_scale):
    values = rows.astype(jnp.float32)
    center = lax.optimization_barrier(jnp.mean(values, axis=1, keepdims=True))
    spread_sq = lax.optimization_barrier(jnp.mean((values - center) ** 2, axis=1, keepdims=True))
    normed = ((values - center) * lax.rsqrt(spread_sq + 1e-06) * norm_gain + norm_bias).astype(jnp.bfloat16)
    hidden = jax.nn.gelu(jnp.dot(normed, fc1_weight, preferred_element_type=jnp.float32) + fc1_bias, approximate=False).astype(jnp.bfloat16)
    partial_value = jnp.dot(hidden, fc2_weight, preferred_element_type=jnp.float32)
    return (values + layer_scale * (partial_value + fc2_bias)).astype(jnp.bfloat16)

def reference(hidden_rows, key_grad, value_grad, visual_rows, visual_cotangent, norm_gain, norm_bias, fc1_weight, fc1_bias, fc2_weight, fc2_bias, layer_scale, token_counts, dest_offsets):
    width = hidden_rows.shape[1]
    blocks = hidden_rows.reshape(N_DP, TOK_DEV, width)
    key_blocks = key_grad.reshape(N_DP, TOK_DEV, KV_WIDTH)
    value_blocks = value_grad.reshape(N_DP, TOK_DEV, KV_WIDTH)

    def accumulate(carry, pieces):
        inputs, key_piece, value_piece = pieces
        key_total, value_total = carry
        key_total = key_total + lax.dot_general(inputs, key_piece, (((0,), (0,)), ((), ())), preferred_element_type=jnp.float32)
        value_total = value_total + lax.dot_general(inputs, value_piece, (((0,), (0,)), ((), ())), preferred_element_type=jnp.float32)
        return ((key_total, value_total), None)
    empty = jnp.zeros((width, KV_WIDTH), jnp.float32)
    (key_total, value_total), _ = lax.scan(accumulate, (empty, empty), (blocks, key_blocks, value_blocks))
    key_bias = lax.optimization_barrier(jnp.sum(key_grad.astype(jnp.float32), axis=0))[None, :]
    value_bias = lax.optimization_barrier(jnp.sum(value_grad.astype(jnp.float32), axis=0))[None, :]
    zero_rows = jnp.zeros((D_PAD - width - 1, KV_WIDTH), jnp.float32)
    key_weight_grad = jnp.concatenate([key_total, key_bias, zero_rows], axis=0)
    value_weight_grad = jnp.concatenate([value_total, value_bias, zero_rows], axis=0)
    encoded = encode(visual_rows, norm_gain, norm_bias, fc1_weight, fc1_bias, fc2_weight, fc2_bias, layer_scale)
    packed = jax.vmap(pack_rows)(encoded.reshape(N_DP, ROWS_DEV, FEAT), token_counts, dest_offsets)
    handoff = jnp.stack([jnp.roll(packed[:, distance], distance + 1, axis=0) for distance in range(SPREAD)], axis=1)
    cot_flat = visual_cotangent.reshape(N_DP * SPREAD * CAP, width)
    rows_flat = handoff.reshape(N_DP * SPREAD * CAP, FEAT)
    projector_main = lax.dot_general(cot_flat, rows_flat, (((0,), (0,)), ((), ())), preferred_element_type=jnp.float32)
    projector_grad = jnp.concatenate([projector_main, jnp.zeros((D_PAD - width, FEAT), jnp.float32)], axis=0)
    return (key_weight_grad, value_weight_grad, projector_grad, handoff)
```

```python
import functools

import jax
import jax.numpy as jnp
from jax import lax
from jax.experimental import pallas as pl
from jax.experimental.pallas import tpu as pltpu
from jax.sharding import PartitionSpec as P

MESH = pl.DeviceIdType.MESH
BF = jnp.bfloat16
F32 = jnp.float32


def up(x, m):
    return -(-x // m) * m


def factors(n):
    core = 2 if n % 2 == 0 else 1
    rest = n // core
    inner = max(f for f in range(1, rest + 1) if rest % f == 0 and f * f <= rest)
    return core, inner, rest // inner


def erf_gelu(x):
    return 0.5 * x * (1.0 + lax.erf(x * (0.5**0.5)))


def kernel(
    cfg,
    hid_h, key_h, val_h, vis_h, cot_h, fc1_h, fc2_h,
    gain, beta, fc1_b, fc2_b, scale, counts, offsets,
    key_o, val_o, proj_o, hand_o,
    hid, key, val, vis, cot, fc1, fc2,
    big_k, big_v, big_c,
    cot_mine, cot_recv,
    k0, k0r, k1, k1r, k2, k2r,
    v0, v0r, v1, v1r, v2, v2r,
    z_own, z_send, z_recv, pack, hbuf, acc, rs_send, rs_recv,
    load_sem, cot_ss, cot_rs, z_ss, z_rs,
    k0_s, k0_r, k1_s, k1_r, k2_s, k2_r,
    v0_s, v0_r, v1_s, v1_r, v2_s, v2_r,
    h_ss, h_rs, p_ss, p_rs,
):
    n, mp, shard, rows_pad, spread, cap, nf = cfg
    nc, na, nb = factors(n)
    chips = n // nc
    me = lax.axis_index("dp")
    col = lax.axis_index("mp")
    dc = lax.rem(me, nc)
    da = lax.rem(lax.div(me, nc), na)
    db = lax.div(me, nc * na)
    chip = lax.div(me, nc)
    tokens, width = hid.shape
    slots = cot.shape[0]
    kc = key.shape[1]
    fcol = hand_o.shape[1]
    fw = fcol // nf

    def rank(c, a, b):
        return (b * na + a) * nc + c

    loads = []
    for i, (src, dst) in enumerate(
        ((vis_h, vis), (fc1_h, fc1), (fc2_h, fc2), (key_h, key), (val_h, val), (hid_h, hid), (cot_h, cot))
    ):
        cp = pltpu.make_async_copy(src, dst, load_sem.at[i])
        cp.start()
        loads.append(cp)
    barrier = pltpu.get_barrier_semaphore()
    for j in range(1, n):
        pl.semaphore_signal(barrier, inc=1, device_id={"dp": lax.rem(me + j, n)}, device_id_type=MESH)
    for j in range(1, mp):
        pl.semaphore_signal(barrier, inc=1, device_id={"mp": lax.rem(col + j, mp)}, device_id_type=MESH)

    def copy_to(src, dst, ss, rs, where):
        return pltpu.make_async_remote_copy(
            src_ref=src, dst_ref=dst, send_sem=ss, recv_sem=rs, device_id=where, device_id_type=MESH
        )

    def remote(src, dst, ss, rs, where):
        cp = copy_to(src, dst, ss, rs, where)
        cp.start()
        return cp

    step = 512 if width % 512 == 0 else 128
    sent = []

    loads[0].wait()
    values = vis[...].astype(F32)
    center = jnp.mean(values, axis=1, keepdims=True)
    cen = values - center
    var = jnp.mean(cen * cen, axis=1, keepdims=True)
    normed = (cen * lax.rsqrt(var + 1e-06) * gain[...] + beta[...]).astype(BF)
    loads[1].wait()
    hidden = erf_gelu(jnp.dot(normed, fc1[...], preferred_element_type=F32) + fc1_b[...]).astype(BF)
    loads[2].wait()

    def feat(i, f=0, w=fcol):
        return pl.ds(pl.multiple_of(i * fcol + f * fw, 128 if fw % 128 == 0 else fw), w)

    order = sorted(range(1, mp), key=lambda j: abs(j - mp / 2))

    def z_copy(f, j):
        return copy_to(
            z_send.at[f, j - 1], z_recv.at[f, j - 1], z_ss.at[f, j - 1], z_rs.at[f, j - 1],
            {"mp": lax.rem(col + j, mp)},
        )

    for i, j in enumerate(order):
        part = jnp.dot(hidden, fc2[:, feat(lax.rem(col + j, mp))], preferred_element_type=F32).astype(BF)
        for f in range(nf):
            z_send[f, j - 1] = part[:, f * fw : (f + 1) * fw]
        if i == 0:
            pl.semaphore_wait(barrier, n - 1 + mp - 1)
        z_copy(0, j).start()
    for f in range(1, nf):
        for j in order:
            z_copy(f, j).start()
    own = jnp.dot(hidden, fc2[:, feat(col)], preferred_element_type=F32)
    for f in range(nf):
        z_own[f] = own[:, f * fw : (f + 1) * fw]

    for cp in loads[3:6]:
        cp.wait()
    kv = jnp.concatenate([key[...], val[...]], axis=1)

    def product(i, _):
        at = pl.multiple_of(i * step, step)
        res = lax.dot_general(hid[:, pl.ds(at, step)], kv, (((0,), (0,)), ((), ())), preferred_element_type=F32)
        big_k[pl.ds(at, step), :] = res[:, :kc]
        big_v[pl.ds(at, step), :] = res[:, kc:]
        return 0

    lax.fori_loop(0, width // step, product, 0)
    tail = big_k.shape[0] - width
    first = lax.broadcasted_iota(jnp.int32, (tail, kc), 0) == 0
    big_k[width:, :] = jnp.where(first, jnp.sum(key[...].astype(F32), axis=0, keepdims=True), 0.0)
    big_v[width:, :] = jnp.where(first, jnp.sum(val[...].astype(F32), axis=0, keepdims=True), 0.0)
    for r in range(n):
        c, a, b = r % nc, (r // nc) % na, r // (nc * na)
        k0[c, a, b] = big_k[r * shard : r * shard + rows_pad, :].astype(BF)
        v0[c, b, a] = big_v[r * shard : r * shard + rows_pad, :].astype(BF)

    def exchange(buf, got, ss, rs, digit, q, peer_of):
        cps = []
        for j in range(1, q):
            to = lax.rem(digit + j, q)
            cps.append(remote(buf.at[to], got.at[j - 1], ss.at[j - 1], rs.at[j - 1], {"dp": peer_of(to)}))
        return cps

    def added(buf, got, digit, q, at):
        total = buf[(digit,) + at].astype(F32)
        for j in range(1, q):
            total = total + got[(j - 1,) + at].astype(F32)
        return total

    at_c = lambda c: rank(c, da, db)
    at_a = lambda a: rank(dc, a, db)
    at_b = lambda b: rank(dc, da, b)
    s0k = exchange(k0, k0r, k0_s, k0_r, dc, nc, at_c)
    s0v = exchange(v0, v0r, v0_s, v0_r, dc, nc, at_c)

    loads[6].wait()
    half = 128

    def turn(i, _):
        at = pl.multiple_of(i * step, step)
        for h in range(slots // half):
            piece = cot[h * half : (h + 1) * half, pl.ds(at, step)].astype(F32)
            big_c[h, pl.ds(at, step), :] = piece.T
        return 0

    lax.fori_loop(0, width // step, turn, 0)
    ctail = big_c.shape[1] - width
    big_c[:, width:, :] = jnp.zeros((slots // half, ctail, half), F32)
    for r in range(n):
        for h in range(slots // half):
            cot_mine[r % nc, r // nc, :, h * half : (h + 1) * half] = big_c[
                h, r * shard : r * shard + rows_pad, :
            ].astype(BF)
    cot_cps = exchange(cot_mine, cot_recv, cot_ss, cot_rs, dc, nc, at_c)

    for cp in s0k:
        cp.wait_recv()
    for a in range(na):
        for b in range(nb):
            k1[a, b] = added(k0, k0r, dc, nc, (a, b)).astype(BF)
    s1k = exchange(k1, k1r, k1_s, k1_r, da, na, at_a)
    for cp in s0v:
        cp.wait_recv()
    for b in range(nb):
        for a in range(na):
            v1[b, a] = added(v0, v0r, dc, nc, (b, a)).astype(BF)
    s1v = exchange(v1, v1r, v1_s, v1_r, db, nb, at_b)

    rows = vis.shape[0]
    images = counts.shape[1]
    place = lax.broadcasted_iota(jnp.int32, (1, rows), 1)
    target = jnp.full((1, rows), -1, jnp.int32)
    start = jnp.int32(0)
    for i in range(images):
        cnt, off = counts[0, i], offsets[0, i]
        before = jnp.int32(0)
        for e in range(i):
            before = before + jnp.where(offsets[0, e] == off, counts[0, e], 0)
        inside = (place >= start) & (place < start + cnt)
        target = jnp.where(inside, (off - 1) * cap + before + place - start, target)
        start = start + cnt
    slot_id = lax.broadcasted_iota(jnp.int32, (spread * cap, rows), 0)
    select = jnp.where(slot_id == target, 1.0, 0.0).astype(BF)

    def hand_copy(f, k, t):
        to = lax.rem(me + k, n)
        inside = lax.rem(to, nc)
        return copy_to(
            pack.at[f, k - 1], hbuf.at[f, inside, k - 1], h_ss.at[f, k - 1, t], h_rs.at[f, inside, k - 1],
            {"dp": lax.div(to, nc) * nc + t},
        )

    def each_hand(f, act):
        for k in range(spread, 0, -1):
            for t in range(nc):
                if k < nc:
                    @pl.when(jnp.logical_not((dc + k < nc) & (dc == t)))
                    def _():
                        act(hand_copy(f, k, t))
                else:
                    act(hand_copy(f, k, t))

    def encode(f):
        for j in range(1, mp):
            z_copy(f, j).wait_recv()
        summed = z_own[f]
        for j in range(1, mp):
            summed = summed + z_recv[f, j - 1].astype(F32)
        at = feat(col, f, fw)
        encoded = (vis[:, at].astype(F32) + scale[:, at] * (summed + fc2_b[:, at])).astype(BF)
        packed = jnp.dot(select, encoded, preferred_element_type=F32).astype(BF)
        for k in range(1, spread + 1):
            pack[f, k - 1] = packed[(k - 1) * cap : k * cap, :]
        for k in range(1, nc):
            for c in range(nc - k):
                @pl.when(dc == c)
                def _():
                    hbuf[f, c + k, k - 1] = packed[(k - 1) * cap : k * cap, :]
        each_hand(f, lambda cp: cp.start())

    def hand_wait(f):
        for k in range(spread, 0, -1):
            for inside in range(nc):
                cp = copy_to(
                    pack.at[f, k - 1], hbuf.at[f, inside, k - 1], h_ss.at[f, k - 1, 0],
                    h_rs.at[f, inside, k - 1], {"dp": lax.rem(me + k, n)},
                )
                if inside >= k:
                    @pl.when(dc != inside - k)
                    def _():
                        cp.wait_recv()
                else:
                    cp.wait_recv()

    offs = [(ja, jb) for jb in range(nb) for ja in range(na) if ja or jb]
    offs.sort(key=lambda o: -((o[0] > 0) + (o[1] > 0)))

    def rs_copy(f, i):
        ja, jb = offs[i]
        to = rank(dc, lax.rem(da + ja, na), lax.rem(db + jb, nb))
        return copy_to(rs_send.at[f, i], rs_recv.at[f, i], p_ss.at[f, i], p_rs.at[f, i], {"dp": to})

    def product_of(f, to):
        got = hbuf[f, dc].reshape(slots, fw)
        total = jnp.dot(cot_mine[dc, to], got, preferred_element_type=F32)
        for j in range(1, nc):
            other = hbuf[f, lax.rem(dc + nc - j, nc)].reshape(slots, fw)
            total = total + jnp.dot(cot_recv[j - 1, to], other, preferred_element_type=F32)
        return total

    def project(f):
        for i, (ja, jb) in enumerate(offs):
            to = lax.rem(db + jb, nb) * na + lax.rem(da + ja, na)
            rs_send[f, i] = product_of(f, to).astype(BF)
            rs_copy(f, i).start()
        acc[f] = product_of(f, chip)

    encode(0)

    for cp in s1k:
        cp.wait_recv()
    for b in range(nb):
        k2[b] = added(k1, k1r, da, na, (b,)).astype(BF)
    s2k = exchange(k2, k2r, k2_s, k2_r, db, nb, at_b)
    for cp in s1v:
        cp.wait_recv()
    for a in range(na):
        v2[a] = added(v1, v1r, db, nb, (a,)).astype(BF)
    s2v = exchange(v2, v2r, v2_s, v2_r, da, na, at_a)

    for cp in cot_cps:
        cp.wait_recv()
    hand_wait(0)
    project(0)
    for f in range(1, nf):
        encode(f)
        hand_wait(f)
        project(f)

    for f in range(nf):
        hand_o[:, f * fw : (f + 1) * fw] = hbuf[f, dc].reshape(slots, fw)
    for cp in s2k:
        cp.wait_recv()
    key_o[...] = added(k2, k2r, db, nb, ())[:shard]
    for cp in s2v:
        cp.wait_recv()
    val_o[...] = added(v2, v2r, da, na, ())[:shard]
    for f in range(nf):
        total = acc[f]
        for i in range(len(offs)):
            rs_copy(f, i).wait_recv()
            total = total + rs_recv[f, i].astype(F32)
        proj_o[:, f * fw : (f + 1) * fw] = total[:shard]

    for f in range(nf):
        for j in range(1, mp):
            z_copy(f, j).wait_send()
        each_hand(f, lambda cp: cp.wait_send())
        for i in range(len(offs)):
            rs_copy(f, i).wait_send()
    for cp in cot_cps + s0k + s0v + s1k + s1v + s2k + s2v:
        cp.wait_send()


def finish(*refs):
    half = len(refs) // 2
    for src, dst in zip(refs[:half], refs[half:]):
        dst[...] = src[...]


def per_device(
    n, mp, hidden_rows, key_grad, value_grad, visual_rows, visual_cotangent, norm_gain, norm_bias,
    fc1_weight, fc1_bias, fc2_weight, fc2_bias, layer_scale, token_counts, dest_offsets,
):
    tokens, width = hidden_rows.shape
    spread, cap = visual_cotangent.shape[1:3]
    slots = spread * cap
    shard = (width + n) // n
    rp = up(shard, 16)
    nc, na, nb = factors(n)
    kc = key_grad.shape[1]
    rows, feats = visual_rows.shape
    fcol = feats // mp
    nf = max(1, fcol // 128)
    fw = fcol // nf
    tall = up(max((n - 1) * shard + rp, width + 8), 8)
    any_spec = pl.BlockSpec(memory_space=pl.ANY)
    vm = pl.BlockSpec(memory_space=pltpu.VMEM)
    sm = pl.BlockSpec(memory_space=pltpu.SMEM)
    dma = lambda *s: pltpu.SemaphoreType.DMA(tuple(max(x, 1) for x in s))

    def stages(q1, q2):
        return [
            pltpu.VMEM((nc, q1, q2, rp, kc), BF),
            pltpu.VMEM((max(nc - 1, 1), q1, q2, rp, kc), BF),
            pltpu.VMEM((q1, q2, rp, kc), BF),
            pltpu.VMEM((max(q1 - 1, 1), q2, rp, kc), BF),
            pltpu.VMEM((q2, rp, kc), BF),
            pltpu.VMEM((max(q2 - 1, 1), rp, kc), BF),
        ]

    def stage_sems(q1, q2):
        return [dma(q - 1) for q in (nc, nc, q1, q1, q2, q2)]

    outs = pl.pallas_call(
        functools.partial(kernel, (n, mp, shard, rp, spread, cap, nf)),
        out_shape=(
            jax.ShapeDtypeStruct((shard, kc), F32),
            jax.ShapeDtypeStruct((shard, kc), F32),
            jax.ShapeDtypeStruct((shard, fcol), F32),
            jax.ShapeDtypeStruct((slots, fcol), BF),
        ),
        in_specs=[any_spec] * 7 + [vm] * 5 + [sm] * 2,
        out_specs=(vm, vm, vm, vm),
        scratch_shapes=[
            pltpu.VMEM(x.shape, BF)
            for x in (hidden_rows, key_grad, value_grad, visual_rows)
        ]
        + [
            pltpu.VMEM((slots, width), BF),
            pltpu.VMEM(fc1_weight.shape, BF),
            pltpu.VMEM(fc2_weight.shape, BF),
            pltpu.VMEM((tall, kc), F32),
            pltpu.VMEM((tall, kc), F32),
            pltpu.VMEM((slots // 128, tall, 128), F32),
            pltpu.VMEM((nc, n // nc, rp, slots), BF),
            pltpu.VMEM((max(nc - 1, 1), n // nc, rp, slots), BF),
        ]
        + stages(na, nb)
        + stages(nb, na)
        + [
            pltpu.VMEM((nf, rows, fw), F32),
            pltpu.VMEM((nf, mp - 1, rows, fw), BF),
            pltpu.VMEM((nf, mp - 1, rows, fw), BF),
            pltpu.VMEM((nf, spread, cap, fw), BF),
            pltpu.VMEM((nf, nc, spread, cap, fw), BF),
            pltpu.VMEM((nf, rp, fw), F32),
            pltpu.VMEM((nf, n // nc - 1, rp, fw), BF),
            pltpu.VMEM((nf, n // nc - 1, rp, fw), BF),
            dma(7), dma(nc - 1), dma(nc - 1), dma(nf, mp - 1), dma(nf, mp - 1),
        ]
        + stage_sems(na, nb)
        + stage_sems(nb, na)
        + [
            dma(nf, spread, nc), dma(nf, nc, spread),
            dma(nf, n // nc - 1), dma(nf, n // nc - 1),
        ],
        compiler_params=pltpu.CompilerParams(
            collective_id=0, has_side_effects=True, vmem_limit_bytes=60 * 1024 * 1024
        ),
    )(
        hidden_rows, key_grad, value_grad, visual_rows, visual_cotangent.reshape(slots, width),
        fc1_weight, fc2_weight, norm_gain[None], norm_bias[None], fc1_bias[None], fc2_bias[None],
        layer_scale[None], token_counts, dest_offsets,
    )
    outs = pl.pallas_call(
        finish,
        out_shape=tuple(jax.ShapeDtypeStruct(x.shape, x.dtype) for x in outs),
        in_specs=[vm] * 4,
        out_specs=(vm,) * 4,
    )(*outs)
    return outs[0], outs[1], outs[2], outs[3].reshape(1, spread, cap, fcol)


def solution(mesh):
    placed = (
        P("dp", None), P("dp", "mp"), P("dp", "mp"), P("dp", None), P("dp", None, None, None),
        P(), P(), P(None, "mp"), P("mp"), P("mp", None), P(), P(), P("dp", None), P("dp", None),
    )
    return jax.shard_map(
        functools.partial(per_device, mesh.shape["dp"], mesh.shape["mp"]),
        mesh=mesh,
        in_specs=placed,
        out_specs=(P("dp", "mp"), P("dp", "mp"), P("dp", "mp"), P("dp", None, None, "mp")),
        check_vma=False,
    )
```

```python
import functools

import jax
import jax.numpy as jnp
from jax import lax
from jax.experimental import pallas as pl
from jax.experimental.pallas import tpu as pltpu
from jax.sharding import PartitionSpec as P

MESH = pl.DeviceIdType.MESH
BF = jnp.bfloat16
F32 = jnp.float32


def up(x, m):
    return -(-x // m) * m


def factors(n):
    core = 2 if n % 2 == 0 else 1
    rest = n // core
    inner = max(f for f in range(1, rest + 1) if rest % f == 0 and f * f <= rest)
    return core, inner, rest // inner


def erf_gelu(x):
    return 0.5 * x * (1.0 + lax.erf(x * (0.5**0.5)))


def kernel(
    cfg,
    hid_h, key_h, val_h, vis_h, cot_h, fc1_h, fc2_h,
    gain_h, beta_h, fc1_bh, fc2_bh, scale_h, counts_h, offsets_h,
    key_o, val_o, proj_o, hand_o,
    hid, key, val, vis, cot, fc1, fc2,
    gain, beta, fc1_b, fc2_b, scale, counts, offsets,
    big_k, big_v, big_c,
    cot_mine, cot_recv,
    k0, k0r, k1, k1r, k2, k2r,
    v0, v0r, v1, v1r, v2, v2r,
    z_full, z_own, z_send, z_recv, z_relay, pack, hbuf, acc, rs_send, rs_recv,
    x1, x1r, x2, x2r, y1, y1r, y2, y2r,
    load_sem, cot_ss, cot_rs, z_ss, z_rs, e_ss, e_rs,
    k0_s, k0_r, k1_s, k1_r, k2_s, k2_r,
    v0_s, v0_r, v1_s, v1_r, v2_s, v2_r,
    h_ss, h_rs, g_ss, g_rs, p_ss, p_rs,
    x1_s, x1_r, x2_s, x2_r, y1_s, y1_r, y2_s, y2_r,
):
    n, mp, shard, rows_pad, spread, cap, nf, groups = cfg
    nc, na, nb = factors(n)
    chips = n // nc
    me = lax.axis_index("dp")
    col = lax.axis_index("mp")
    dc = lax.rem(me, nc)
    da = lax.rem(lax.div(me, nc), na)
    db = lax.div(me, nc * na)
    chip = lax.div(me, nc)
    tokens, width = hid.shape
    slots = cot.shape[0]
    kc = key.shape[1]
    fcol = hand_o.shape[1]
    fw = fcol // nf

    def rank(c, a, b):
        return (b * na + a) * nc + c

    loads = []
    for i, (src, dst) in enumerate(
        (
            (vis_h, vis), (gain_h, gain), (beta_h, beta), (fc1_h, fc1), (fc1_bh, fc1_b), (fc2_h, fc2),
            (key_h, key), (val_h, val), (hid_h, hid), (cot_h, cot),
            (fc2_bh, fc2_b), (scale_h, scale), (counts_h, counts), (offsets_h, offsets),
        )
    ):
        cp = pltpu.make_async_copy(src, dst, load_sem.at[i])
        cp.start()
        loads.append(cp)
    barrier = pltpu.get_barrier_semaphore()
    for j in range(1, n):
        pl.semaphore_signal(barrier, inc=1, device_id={"dp": lax.rem(me + j, n)}, device_id_type=MESH)
    for j in range(1, mp):
        pl.semaphore_signal(barrier, inc=1, device_id={"mp": lax.rem(col + j, mp)}, device_id_type=MESH)

    def copy_to(src, dst, ss, rs, where):
        return pltpu.make_async_remote_copy(
            src_ref=src, dst_ref=dst, send_sem=ss, recv_sem=rs, device_id=where, device_id_type=MESH
        )

    def remote(src, dst, ss, rs, where):
        cp = copy_to(src, dst, ss, rs, where)
        cp.start()
        return cp

    loads[0].wait()
    values = vis[...].astype(F32)
    center = jnp.mean(values, axis=1, keepdims=True)
    cen = values - center
    var = jnp.mean(cen * cen, axis=1, keepdims=True)
    for cp in loads[1:3]:
        cp.wait()
    normed = (cen * lax.rsqrt(var + 1e-06) * gain[...] + beta[...]).astype(BF)
    for cp in loads[3:5]:
        cp.wait()
    hidden = erf_gelu(jnp.dot(normed, fc1[...], preferred_element_type=F32) + fc1_b[...]).astype(BF)
    loads[5].wait()
    partial = jnp.dot(hidden, fc2[...], preferred_element_type=F32)
    for m in range(mp):
        for f in range(nf):
            piece = partial[:, m * fcol + f * fw : m * fcol + (f + 1) * fw]
            z_full[f, m] = piece
            z_send[f, m] = piece.astype(BF)

    def feat(i, f=0, w=fcol):
        return pl.ds(pl.multiple_of(i * fcol + f * fw, 128 if fw % 128 == 0 else fw), w)

    chain = mp >= 4
    low, high = col == 0, col == mp - 1
    if chain:
        edge = low | high
        near = jnp.where(low, 1, mp - 2)
        inner = (col == 1) | (col == mp - 2)
        beyond = jnp.where(col == 1, mp - 1, 0)
        opposite = jnp.where(low, mp - 1, 0)
    order = sorted(range(1, mp), key=lambda j: abs(j - mp / 2))

    def z_copy(f, j):
        to = lax.rem(col + j, mp)
        return copy_to(z_send.at[f, to], z_recv.at[f, j - 1], z_ss.at[f, j - 1], z_rs.at[f, j - 1], {"mp": to})

    def e_copy(f):
        return copy_to(z_send.at[f, opposite], z_relay.at[f], e_ss.at[f], e_rs.at[f], {"mp": near})

    def r_copy(f):
        j = jnp.where(col == 1, mp - 2, 2)
        return copy_to(z_send.at[f, beyond], z_recv.at[f, j - 1], z_ss.at[f, j - 1], z_rs.at[f, j - 1], {"mp": beyond})

    def held(j):
        to = lax.rem(col + j, mp)
        return (low & (to == mp - 1)) | (high & (to == 0)), ((col == 1) & (to == mp - 1)) | ((col == mp - 2) & (to == 0))

    def z_start(f):
        for j in order:
            if chain:
                skip, later = held(j)

                @pl.when(jnp.logical_not(skip | later))
                def _():
                    z_copy(f, j).start()
            else:
                z_copy(f, j).start()

    def z_pass(f):
        if chain:
            @pl.when(inner)
            def _():
                e_copy(f).wait_recv()
                z_send[f, beyond] = (z_full[f, beyond] + z_relay[f].astype(F32)).astype(BF)
                r_copy(f).start()

    def z_sum(f):
        z_own[f] = z_full[f, col]
        for j in order:
            def take():
                z_copy(f, j).wait_recv()
                z_own[f] += z_recv[f, j - 1].astype(F32)

            source = lax.rem(col + mp - j, mp)
            if chain:
                @pl.when(jnp.logical_not((low & (source == mp - 1)) | (high & (source == 0))))
                def _():
                    take()
            else:
                take()

    def z_drain(f):
        if chain:
            @pl.when(edge)
            def _():
                e_copy(f).wait_send()
        for j in order:
            if chain:
                skip, _ = held(j)

                @pl.when(jnp.logical_not(skip))
                def _():
                    z_copy(f, j).wait_send()
            else:
                z_copy(f, j).wait_send()

    pl.semaphore_wait(barrier, n - 1 + mp - 1)
    if chain:
        @pl.when(edge)
        def _():
            for f in range(nf):
                e_copy(f).start()
    for f in range(nf):
        z_start(f)

    for cp in loads[6:9]:
        cp.wait()
    kv = jnp.concatenate([key[...], val[...]], axis=1)
    tail = big_k.shape[0] - width
    first = lax.broadcasted_iota(jnp.int32, (tail, kc), 0) == 0
    big_k[width:, :] = jnp.where(first, jnp.sum(key[...].astype(F32), axis=0, keepdims=True), 0.0)
    big_v[width:, :] = jnp.where(first, jnp.sum(val[...].astype(F32), axis=0, keepdims=True), 0.0)
    nbg = nb // groups
    at_c = lambda c: rank(c, da, db)
    at_a = lambda a: rank(dc, a, db)
    at_b = lambda b: rank(dc, da, b)

    def kv_first(buf, got, ss, rs, g):
        part = pl.ds(g * nbg, nbg)
        cps = []
        for j in range(1, nc):
            to = lax.rem(dc + j, nc)
            cps.append(copy_to(buf.at[to, part], got.at[j - 1, part], ss.at[j - 1, g], rs.at[j - 1, g], {"dp": at_c(to)}))
        return cps

    block = width if groups == 1 else min(width, up((nbg * na * nc - 1) * shard + rows_pad, 128))
    stride = 0 if groups == 1 else (width - block) // (groups - 1)

    def product(i, _):
        at = pl.multiple_of(i * stride, 128)
        res = lax.dot_general(
            hid[:, pl.ds(at, block)], kv, (((0,), (0,)), ((), ())), preferred_element_type=F32
        )
        big_k[pl.ds(at, block), :] = res[:, :kc]
        big_v[pl.ds(at, block), :] = res[:, kc:]
        for g in range(groups):
            @pl.when(i == g)
            def _():
                for b in range(g * nbg, (g + 1) * nbg):
                    for a in range(na):
                        for c in range(nc):
                            r = rank(c, a, b)
                            k0[c, b, a] = big_k[r * shard : r * shard + rows_pad, :].astype(BF)
                            v0[c, b, a] = big_v[r * shard : r * shard + rows_pad, :].astype(BF)
                for cp in kv_first(k0, k0r, k0_s, k0_r, g) + kv_first(v0, v0r, v0_s, v0_r, g):
                    cp.start()
        return 0

    lax.fori_loop(0, groups, product, 0)

    def exchange(buf, got, ss, rs, digit, q, peer_of):
        cps = []
        for j in range(1, q):
            to = lax.rem(digit + j, q)
            cps.append(copy_to(buf.at[to], got.at[j - 1], ss.at[j - 1], rs.at[j - 1], {"dp": peer_of(to)}))
        return cps

    def begin(cps):
        for cp in cps:
            cp.start()
        return cps

    def added(buf, got, digit, q, at):
        total = buf[(digit,) + at].astype(F32)
        for j in range(1, q):
            total = total + got[(j - 1,) + at].astype(F32)
        return total

    loads[9].wait()
    half = 128
    step = width // 2 if width % 256 == 0 else 128

    def turn(i, _):
        at = pl.multiple_of(i * step, 128)
        for h in range(slots // half):
            piece = cot[h * half : (h + 1) * half, pl.ds(at, step)].astype(F32)
            big_c[h, pl.ds(at, step), :] = piece.T
        return 0

    lax.fori_loop(0, width // step, turn, 0)

    def kv_second(g):
        for b in range(g * nbg, (g + 1) * nbg):
            for a in range(na):
                k1[a, b] = added(k0, k0r, dc, nc, (b, a)).astype(BF)
                v1[b, a] = added(v0, v0r, dc, nc, (b, a)).astype(BF)
        part = pl.ds(g * nbg, nbg)
        for j in range(1, na):
            k1_copy(j, g).start()
        for j in range(1, nb):
            @pl.when(lax.div(lax.rem(db + j, nb), nbg) == g)
            def _():
                v1_copy(j).start()

    def k1_copy(j, g):
        part = pl.ds(g * nbg, nbg)
        to = lax.rem(da + j, na)
        return copy_to(k1.at[to, part], k1r.at[j - 1, part], k1_s.at[j - 1, g], k1_r.at[j - 1, g], {"dp": at_a(to)})

    def v1_copy(j):
        to = lax.rem(db + j, nb)
        return copy_to(v1.at[to], v1r.at[j - 1], v1_s.at[j - 1], v1_r.at[j - 1], {"dp": at_b(to)})

    for g in range(groups):
        for cp in kv_first(k0, k0r, k0_s, k0_r, g) + kv_first(v0, v0r, v0_s, v0_r, g):
            cp.wait_recv()
        kv_second(g)
        if g == 0:
            z_pass(0)

    ctail = big_c.shape[1] - width
    big_c[:, width:, :] = jnp.zeros((slots // half, ctail, half), F32)
    for r in range(n):
        for h in range(slots // half):
            cot_mine[r % nc, r // nc, :, h * half : (h + 1) * half] = big_c[
                h, r * shard : r * shard + rows_pad, :
            ].astype(BF)
    cot_cps = begin(exchange(cot_mine, cot_recv, cot_ss, cot_rs, dc, nc, at_c))

    for cp in loads[10:]:
        cp.wait()
    rows = vis.shape[0]
    images = counts.shape[1]
    place = lax.broadcasted_iota(jnp.int32, (1, rows), 1)
    target = jnp.full((1, rows), -1, jnp.int32)
    start = jnp.int32(0)
    for i in range(images):
        cnt, off = counts[0, i], offsets[0, i]
        before = jnp.int32(0)
        for e in range(i):
            before = before + jnp.where(offsets[0, e] == off, counts[0, e], 0)
        inside = (place >= start) & (place < start + cnt)
        target = jnp.where(inside, (off - 1) * cap + before + place - start, target)
        start = start + cnt
    slot_id = lax.broadcasted_iota(jnp.int32, (spread * cap, rows), 0)
    select = jnp.where(slot_id == target, 1.0, 0.0).astype(BF)

    def hand_copy(f, k):
        to = lax.rem(me + k, n)
        inside = lax.rem(to, nc)
        return copy_to(pack.at[f, k - 1], hbuf.at[f, inside, k - 1], h_ss.at[f, k - 1], h_rs.at[f, k - 1], {"dp": to})

    def share_copy(f, k, j):
        to = lax.rem(dc + j, nc)
        block = hbuf.at[f, dc, k - 1]
        return copy_to(block, block, g_ss.at[f, k - 1, j - 1], g_rs.at[f, k - 1, j - 1], {"dp": at_c(to)})

    def encode(f):
        z_sum(f)
        at = feat(col, f, fw)
        encoded = (vis[:, at].astype(F32) + scale[:, at] * (z_own[f] + fc2_b[:, at])).astype(BF)
        packed = jnp.dot(select, encoded, preferred_element_type=F32).astype(BF)
        for k in range(1, spread + 1):
            pack[f, k - 1] = packed[(k - 1) * cap : k * cap, :]
        for k in range(spread, 0, -1):
            hand_copy(f, k).start()

    def hand_wait(f):
        for k in range(1, spread + 1):
            hand_copy(f, k).wait_recv()
            for j in range(1, nc):
                share_copy(f, k, j).start()
        for k in range(1, spread + 1):
            for j in range(1, nc):
                share_copy(f, k, j).wait_recv()

    offs = [(ja, jb) for jb in range(nb) for ja in range(na) if ja or jb]
    offs.sort(key=lambda o: -((o[0] > 0) + (o[1] > 0)))

    def rs_copy(i):
        ja, jb = offs[i]
        to = lax.rem(db + jb, nb) * na + lax.rem(da + ja, na)
        return copy_to(rs_send.at[to], rs_recv.at[i], p_ss.at[i], p_rs.at[i], {"dp": to * nc + dc})

    def product_of(f, to):
        got = hbuf[f, dc].reshape(slots, fw)
        total = jnp.dot(cot_mine[dc, to], got, preferred_element_type=F32)
        for j in range(1, nc):
            other = hbuf[f, lax.rem(dc + nc - j, nc)].reshape(slots, fw)
            total = total + jnp.dot(cot_recv[j - 1, to], other, preferred_element_type=F32)
        return total

    top = x1.shape[-2]

    def staged(f):
        for a in range(na):
            for b in range(nb):
                total = product_of(f, b * na + a).astype(BF)
                x1[f, a, b] = total[:top]
                y1[f, b, a] = total[top:]
        return begin(x_first(f) + y_first(f))

    def x_first(f):
        return exchange(x1.at[f], x1r.at[f], x1_s.at[f], x1_r.at[f], da, na, at_a)

    def y_first(f):
        return exchange(y1.at[f], y1r.at[f], y1_s.at[f], y1_r.at[f], db, nb, at_b)

    def x_second(f):
        return exchange(x2.at[f], x2r.at[f], x2_s.at[f], x2_r.at[f], db, nb, at_b)

    def y_second(f):
        return exchange(y2.at[f], y2r.at[f], y2_s.at[f], y2_r.at[f], da, na, at_a)

    def staged_next(f):
        for cp in x_first(f):
            cp.wait_recv()
        for b in range(nb):
            x2[f, b] = added(x1.at[f], x1r.at[f], da, na, (b,)).astype(BF)
        begin(x_second(f))
        for cp in y_first(f):
            cp.wait_recv()
        for a in range(na):
            y2[f, a] = added(y1.at[f], y1r.at[f], db, nb, (a,)).astype(BF)
        begin(y_second(f))

    def direct(f):
        for to in range(chips):
            total = product_of(f, to)
            acc[to] = total
            rs_send[to] = total.astype(BF)
        for i in range(len(offs)):
            rs_copy(i).start()

    for f in range(1, nf):
        z_pass(f)
    for f in range(nf):
        encode(f)

    for g in range(groups):
        for j in range(1, na):
            k1_copy(j, g).wait_recv()
    for b in range(nb):
        k2[b] = added(k1, k1r, da, na, (b,)).astype(BF)
    s2k = begin(exchange(k2, k2r, k2_s, k2_r, db, nb, at_b))
    for j in range(1, nb):
        v1_copy(j).wait_recv()
    for a in range(na):
        v2[a] = added(v1, v1r, db, nb, (a,)).astype(BF)
    s2v = begin(exchange(v2, v2r, v2_s, v2_r, da, na, at_a))

    for cp in cot_cps:
        cp.wait_recv()
    for f in range(nf - 1):
        hand_wait(f)
        staged(f)
    hand_wait(nf - 1)
    direct(nf - 1)
    for f in range(nf - 1):
        staged_next(f)

    for f in range(nf):
        hand_o[:, f * fw : (f + 1) * fw] = hbuf[f, dc].reshape(slots, fw)
    for cp in s2k:
        cp.wait_recv()
    key_o[...] = added(k2, k2r, db, nb, ())[:shard]
    for cp in s2v:
        cp.wait_recv()
    val_o[...] = added(v2, v2r, da, na, ())[:shard]
    total = acc[chip]
    for i in range(len(offs)):
        rs_copy(i).wait_recv()
        total = total + rs_recv[i].astype(F32)
    proj_o[:, (nf - 1) * fw :] = total[:shard]
    for f in range(nf - 1):
        for cp in x_second(f):
            cp.wait_recv()
        proj_o[:top, f * fw : (f + 1) * fw] = added(x2.at[f], x2r.at[f], db, nb, ())
        for cp in y_second(f):
            cp.wait_recv()
        proj_o[top:, f * fw : (f + 1) * fw] = added(y2.at[f], y2r.at[f], da, na, ())[: shard - top]

    for f in range(nf):
        z_drain(f)
        for k in range(1, spread + 1):
            hand_copy(f, k).wait_send()
            for j in range(1, nc):
                share_copy(f, k, j).wait_send()
    for f in range(nf - 1):
        for cp in x_first(f) + y_first(f) + x_second(f) + y_second(f):
            cp.wait_send()
    for i in range(len(offs)):
        rs_copy(i).wait_send()
    for g in range(groups):
        for cp in kv_first(k0, k0r, k0_s, k0_r, g) + kv_first(v0, v0r, v0_s, v0_r, g):
            cp.wait_send()
        for j in range(1, na):
            k1_copy(j, g).wait_send()
    for j in range(1, nb):
        v1_copy(j).wait_send()
    for cp in cot_cps + s2k + s2v:
        cp.wait_send()


def finish(*refs):
    half = len(refs) // 2
    sems = refs[-1]
    cps = []
    for i, (src, dst) in enumerate(zip(refs[:half], refs[half:-1])):
        cp = pltpu.make_async_copy(src, dst, sems.at[i])
        cp.start()
        cps.append(cp)
    for cp in cps:
        cp.wait()


def per_device(
    n, mp, hidden_rows, key_grad, value_grad, visual_rows, visual_cotangent, norm_gain, norm_bias,
    fc1_weight, fc1_bias, fc2_weight, fc2_bias, layer_scale, token_counts, dest_offsets,
):
    tokens, width = hidden_rows.shape
    spread, cap = visual_cotangent.shape[1:3]
    slots = spread * cap
    shard = (width + n) // n
    rp = up(shard, 16)
    nc, na, nb = factors(n)
    chips = n // nc
    kc = key_grad.shape[1]
    rows, feats = visual_rows.shape
    fcol = feats // mp
    nf = max(1, fcol // 128)
    fw = fcol // nf
    groups = 2 if nb % 2 == 0 else 1
    tall = up(max((n - 1) * shard + rp, width + 8), 8)
    top = max(up(rp // 2, 16), 16)
    low = max(rp - top, 16)
    ns = max(nf - 1, 1)
    any_spec = pl.BlockSpec(memory_space=pl.ANY)
    vm = pl.BlockSpec(memory_space=pltpu.VMEM)
    dma = lambda *s: pltpu.SemaphoreType.DMA(tuple(max(x, 1) for x in s))
    bf = lambda *s: pltpu.VMEM(tuple(max(x, 1) for x in s), BF)

    def stages(q1, q2):
        return [
            bf(nc, nb, na, rp, kc), bf(nc - 1, nb, na, rp, kc),
            bf(q1, q2, rp, kc), bf(q1 - 1, q2, rp, kc),
            bf(q2, rp, kc), bf(q2 - 1, rp, kc),
        ]

    def halves(q1, q2, h):
        return [bf(ns, q1, q2, h, fw), bf(ns, q1 - 1, q2, h, fw), bf(ns, q2, h, fw), bf(ns, q2 - 1, h, fw)]

    small = (norm_gain, norm_bias, fc1_bias, fc2_bias, layer_scale)
    outs = pl.pallas_call(
        functools.partial(kernel, (n, mp, shard, rp, spread, cap, nf, groups)),
        out_shape=(
            pltpu.VMEM((shard, kc), F32),
            pltpu.VMEM((shard, kc), F32),
            pltpu.VMEM((shard, fcol), F32),
            pltpu.VMEM((slots, fcol), BF),
        ),
        in_specs=[any_spec] * 14,
        out_specs=(vm, vm, vm, vm),
        scratch_shapes=[
            pltpu.VMEM(x.shape, BF)
            for x in (hidden_rows, key_grad, value_grad, visual_rows)
        ]
        + [bf(slots, width), bf(*fc1_weight.shape), bf(*fc2_weight.shape)]
        + [pltpu.VMEM((1, x.shape[0]), F32) for x in small]
        + [pltpu.SMEM(token_counts.shape, jnp.int32), pltpu.SMEM(dest_offsets.shape, jnp.int32)]
        + [
            pltpu.VMEM((tall, kc), F32),
            pltpu.VMEM((tall, kc), F32),
            pltpu.VMEM((slots // 128, tall, 128), F32),
            bf(nc, chips, rp, slots),
            bf(nc - 1, chips, rp, slots),
        ]
        + stages(na, nb)
        + stages(nb, na)
        + [
            pltpu.VMEM((nf, mp, rows, fw), F32),
            pltpu.VMEM((nf, rows, fw), F32),
            bf(nf, mp, rows, fw),
            bf(nf, mp - 1, rows, fw),
            bf(nf, rows, fw),
            bf(nf, spread, cap, fw),
            bf(nf, nc, spread, cap, fw),
            pltpu.VMEM((chips, rp, fw), F32),
            bf(chips, rp, fw),
            bf(chips - 1, rp, fw),
        ]
        + halves(na, nb, top)
        + halves(nb, na, low)
        + [dma(14), dma(nc - 1), dma(nc - 1), dma(nf, mp - 1), dma(nf, mp - 1), dma(nf), dma(nf)]
        + [dma(nc - 1, groups), dma(nc - 1, groups), dma(na - 1, groups), dma(na - 1, groups), dma(nb - 1), dma(nb - 1)]
        + [dma(nc - 1, groups), dma(nc - 1, groups), dma(nb - 1), dma(nb - 1), dma(na - 1), dma(na - 1)]
        + [dma(nf, spread), dma(nf, spread), dma(nf, spread, nc - 1), dma(nf, spread, nc - 1)]
        + [dma(chips - 1), dma(chips - 1)]
        + [dma(ns, q) for q in (na - 1, na - 1, nb - 1, nb - 1)]
        + [dma(ns, q) for q in (nb - 1, nb - 1, na - 1, na - 1)],
        compiler_params=pltpu.CompilerParams(
            collective_id=0, has_side_effects=True, vmem_limit_bytes=56 * 1024 * 1024
        ),
    )(
        hidden_rows, key_grad, value_grad, visual_rows, visual_cotangent.reshape(slots, width),
        fc1_weight, fc2_weight, *(x[None] for x in small), token_counts, dest_offsets,
    )
    outs = pl.pallas_call(
        finish,
        out_shape=tuple(jax.ShapeDtypeStruct(x.shape, x.dtype) for x in outs),
        in_specs=[vm] * 4,
        out_specs=(any_spec,) * 4,
        scratch_shapes=[dma(4)],
    )(*(pltpu.with_memory_space_constraint(x, pltpu.VMEM) for x in outs))
    return outs[0], outs[1], outs[2], outs[3].reshape(1, spread, cap, fcol)


def solution(mesh):
    placed = (
        P("dp", None), P("dp", "mp"), P("dp", "mp"), P("dp", None), P("dp", None, None, None),
        P(), P(), P(None, "mp"), P("mp"), P("mp", None), P(), P(), P("dp", None), P("dp", None),
    )
    return jax.shard_map(
        functools.partial(per_device, mesh.shape["dp"], mesh.shape["mp"]),
        mesh=mesh,
        in_specs=placed,
        out_specs=(P("dp", "mp"), P("dp", "mp"), P("dp", "mp"), P("dp", None, None, "mp")),
        check_vma=False,
    )
```

```python
import functools

import jax
import jax.numpy as jnp
from jax import lax
from jax.experimental import pallas as pl
from jax.experimental.pallas import tpu as pltpu
from jax.sharding import PartitionSpec as P

MESH = pl.DeviceIdType.MESH
BF = jnp.bfloat16
F32 = jnp.float32


def up(x, m):
    return -(-x // m) * m


def factors(n):
    core = 2 if n % 2 == 0 else 1
    rest = n // core
    inner = max(f for f in range(1, rest + 1) if rest % f == 0 and f * f <= rest)
    return core, inner, rest // inner


def erf_gelu(x):
    return 0.5 * x * (1.0 + lax.erf(x * (0.5**0.5)))


def kernel(
    cfg,
    hid_h, key_h, val_h, vis_h, cot_h, fc1_h, fc2_h,
    gain_h, beta_h, fc1_bh, fc2_bh, scale_h, counts_h, offsets_h,
    key_o, val_o, proj_o, hand_o,
    hid, key, val, vis, cot, fc1, fc2,
    gain, beta, fc1_b, fc2_b, scale, counts, offsets,
    big_k, big_v, big_c,
    cot_mine, cot_recv,
    k0, k0r, k1, k1r, k2, k2r,
    v0, v0r, v1, v1r, v2, v2r,
    z_full, z_own, z_send, z_recv, z_relay, pack, hbuf,
    x1, x1r, x2, x2r, y1, y1r, y2, y2r,
    load_sem, cot_ss, cot_rs, z_ss, z_rs, e_ss, e_rs,
    k0_s, k0_r, k1_s, k1_r, k2_s, k2_r,
    v0_s, v0_r, v1_s, v1_r, v2_s, v2_r,
    h_ss, h_rs, g_ss, g_rs,
    x1_s, x1_r, x2_s, x2_r, y1_s, y1_r, y2_s, y2_r,
):
    n, mp, shard, rows_pad, spread, cap, nf, groups = cfg
    nc, na, nb = factors(n)
    chips = n // nc
    me = lax.axis_index("dp")
    col = lax.axis_index("mp")
    dc = lax.rem(me, nc)
    da = lax.rem(lax.div(me, nc), na)
    db = lax.div(me, nc * na)
    chip = lax.div(me, nc)
    tokens, width = hid.shape
    slots = cot.shape[0]
    kc = key.shape[1]
    fcol = hand_o.shape[1]
    fw = fcol // nf

    def rank(c, a, b):
        return (b * na + a) * nc + c

    loads = []
    for i, (src, dst) in enumerate(
        (
            (vis_h, vis), (gain_h, gain), (beta_h, beta), (fc1_h, fc1), (fc1_bh, fc1_b), (fc2_h, fc2),
            (key_h, key), (val_h, val), (hid_h, hid), (cot_h, cot),
            (fc2_bh, fc2_b), (scale_h, scale), (counts_h, counts), (offsets_h, offsets),
        )
    ):
        cp = pltpu.make_async_copy(src, dst, load_sem.at[i])
        cp.start()
        loads.append(cp)
    barrier = pltpu.get_barrier_semaphore()
    for j in range(1, n):
        pl.semaphore_signal(barrier, inc=1, device_id={"dp": lax.rem(me + j, n)}, device_id_type=MESH)
    for j in range(1, mp):
        pl.semaphore_signal(barrier, inc=1, device_id={"mp": lax.rem(col + j, mp)}, device_id_type=MESH)

    def copy_to(src, dst, ss, rs, where):
        return pltpu.make_async_remote_copy(
            src_ref=src, dst_ref=dst, send_sem=ss, recv_sem=rs, device_id=where, device_id_type=MESH
        )

    def remote(src, dst, ss, rs, where):
        cp = copy_to(src, dst, ss, rs, where)
        cp.start()
        return cp

    loads[0].wait()
    values = vis[...].astype(F32)
    center = jnp.mean(values, axis=1, keepdims=True)
    cen = values - center
    var = jnp.mean(cen * cen, axis=1, keepdims=True)
    for cp in loads[1:3]:
        cp.wait()
    normed = (cen * lax.rsqrt(var + 1e-06) * gain[...] + beta[...]).astype(BF)
    for cp in loads[3:5]:
        cp.wait()
    hidden = erf_gelu(jnp.dot(normed, fc1[...], preferred_element_type=F32) + fc1_b[...]).astype(BF)
    loads[5].wait()
    partial = jnp.dot(hidden, fc2[...], preferred_element_type=F32)
    for m in range(mp):
        for f in range(nf):
            piece = partial[:, m * fcol + f * fw : m * fcol + (f + 1) * fw]
            z_full[f, m] = piece
            z_send[f, m] = piece.astype(BF)

    def feat(i, f=0, w=fcol):
        return pl.ds(pl.multiple_of(i * fcol + f * fw, 128 if fw % 128 == 0 else fw), w)

    chain = mp >= 4
    low, high = col == 0, col == mp - 1
    if chain:
        edge = low | high
        near = jnp.where(low, 1, mp - 2)
        inner = (col == 1) | (col == mp - 2)
        beyond = jnp.where(col == 1, mp - 1, 0)
        opposite = jnp.where(low, mp - 1, 0)
    order = sorted(range(1, mp), key=lambda j: abs(j - mp / 2))

    def z_copy(f, j):
        to = lax.rem(col + j, mp)
        return copy_to(z_send.at[f, to], z_recv.at[f, j - 1], z_ss.at[f, j - 1], z_rs.at[f, j - 1], {"mp": to})

    def e_copy(f):
        return copy_to(z_send.at[f, opposite], z_relay.at[f], e_ss.at[f], e_rs.at[f], {"mp": near})

    def r_copy(f):
        j = jnp.where(col == 1, mp - 2, 2)
        return copy_to(z_send.at[f, beyond], z_recv.at[f, j - 1], z_ss.at[f, j - 1], z_rs.at[f, j - 1], {"mp": beyond})

    def held(j):
        to = lax.rem(col + j, mp)
        return (low & (to == mp - 1)) | (high & (to == 0)), ((col == 1) & (to == mp - 1)) | ((col == mp - 2) & (to == 0))

    def z_start(f):
        for j in order:
            if chain:
                skip, later = held(j)

                @pl.when(jnp.logical_not(skip | later))
                def _():
                    z_copy(f, j).start()
            else:
                z_copy(f, j).start()

    def z_pass(f):
        if chain:
            @pl.when(inner)
            def _():
                e_copy(f).wait_recv()
                z_send[f, beyond] = (z_full[f, beyond] + z_relay[f].astype(F32)).astype(BF)
                r_copy(f).start()

    def z_sum(f):
        z_own[f] = z_full[f, col]
        for j in order:
            def take():
                z_copy(f, j).wait_recv()
                z_own[f] += z_recv[f, j - 1].astype(F32)

            source = lax.rem(col + mp - j, mp)
            if chain:
                @pl.when(jnp.logical_not((low & (source == mp - 1)) | (high & (source == 0))))
                def _():
                    take()
            else:
                take()

    def z_drain(f):
        if chain:
            @pl.when(edge)
            def _():
                e_copy(f).wait_send()
        for j in order:
            if chain:
                skip, _ = held(j)

                @pl.when(jnp.logical_not(skip))
                def _():
                    z_copy(f, j).wait_send()
            else:
                z_copy(f, j).wait_send()

    pl.semaphore_wait(barrier, n - 1 + mp - 1)
    if chain:
        @pl.when(edge)
        def _():
            for f in range(nf):
                e_copy(f).start()
    for f in range(nf):
        z_start(f)

    for cp in loads[6:9]:
        cp.wait()
    kv = jnp.concatenate([key[...], val[...]], axis=1)
    tail = big_k.shape[0] - width
    first = lax.broadcasted_iota(jnp.int32, (tail, kc), 0) == 0
    big_k[width:, :] = jnp.where(first, jnp.sum(key[...].astype(F32), axis=0, keepdims=True), 0.0)
    big_v[width:, :] = jnp.where(first, jnp.sum(val[...].astype(F32), axis=0, keepdims=True), 0.0)
    nbg = nb // groups
    at_c = lambda c: rank(c, da, db)
    at_a = lambda a: rank(dc, a, db)
    at_b = lambda b: rank(dc, da, b)

    def kv_first(buf, got, ss, rs, g):
        part = pl.ds(g * nbg, nbg)
        cps = []
        for j in range(1, nc):
            to = lax.rem(dc + j, nc)
            cps.append(copy_to(buf.at[to, part], got.at[j - 1, part], ss.at[j - 1, g], rs.at[j - 1, g], {"dp": at_c(to)}))
        return cps

    block = width if groups == 1 else min(width, up((nbg * na * nc - 1) * shard + rows_pad, 128))
    stride = 0 if groups == 1 else (width - block) // (groups - 1)

    def product(i, _):
        at = pl.multiple_of(i * stride, 128)
        res = lax.dot_general(
            hid[:, pl.ds(at, block)], kv, (((0,), (0,)), ((), ())), preferred_element_type=F32
        )
        big_k[pl.ds(at, block), :] = res[:, :kc]
        big_v[pl.ds(at, block), :] = res[:, kc:]
        for g in range(groups):
            @pl.when(i == g)
            def _():
                for b in range(g * nbg, (g + 1) * nbg):
                    for a in range(na):
                        for c in range(nc):
                            r = rank(c, a, b)
                            k0[c, b, a] = big_k[r * shard : r * shard + rows_pad, :].astype(BF)
                            v0[c, b, a] = big_v[r * shard : r * shard + rows_pad, :].astype(BF)
                for cp in kv_first(k0, k0r, k0_s, k0_r, g) + kv_first(v0, v0r, v0_s, v0_r, g):
                    cp.start()
        return 0

    lax.fori_loop(0, groups, product, 0)

    def exchange(buf, got, ss, rs, digit, q, peer_of):
        cps = []
        for j in range(1, q):
            to = lax.rem(digit + j, q)
            cps.append(copy_to(buf.at[to], got.at[j - 1], ss.at[j - 1], rs.at[j - 1], {"dp": peer_of(to)}))
        return cps

    def begin(cps):
        for cp in cps:
            cp.start()
        return cps

    def added(buf, got, digit, q, at):
        total = buf[(digit,) + at].astype(F32)
        for j in range(1, q):
            total = total + got[(j - 1,) + at].astype(F32)
        return total

    loads[9].wait()
    half = 128
    step = width // 2 if width % 256 == 0 else 128

    def turn(i, _):
        at = pl.multiple_of(i * step, 128)
        for h in range(slots // half):
            piece = cot[h * half : (h + 1) * half, pl.ds(at, step)].astype(F32)
            big_c[h, pl.ds(at, step), :] = piece.T
        return 0

    lax.fori_loop(0, width // step, turn, 0)

    def kv_second(g):
        for b in range(g * nbg, (g + 1) * nbg):
            for a in range(na):
                k1[a, b] = added(k0, k0r, dc, nc, (b, a)).astype(BF)
                v1[b, a] = added(v0, v0r, dc, nc, (b, a)).astype(BF)
        part = pl.ds(g * nbg, nbg)
        for j in range(1, na):
            k1_copy(j, g).start()
        for j in range(1, nb):
            @pl.when(lax.div(lax.rem(db + j, nb), nbg) == g)
            def _():
                v1_copy(j).start()

    def k1_copy(j, g):
        part = pl.ds(g * nbg, nbg)
        to = lax.rem(da + j, na)
        return copy_to(k1.at[to, part], k1r.at[j - 1, part], k1_s.at[j - 1, g], k1_r.at[j - 1, g], {"dp": at_a(to)})

    def v1_copy(j):
        to = lax.rem(db + j, nb)
        return copy_to(v1.at[to], v1r.at[j - 1], v1_s.at[j - 1], v1_r.at[j - 1], {"dp": at_b(to)})

    for g in range(groups):
        for cp in kv_first(k0, k0r, k0_s, k0_r, g) + kv_first(v0, v0r, v0_s, v0_r, g):
            cp.wait_recv()
        kv_second(g)
        if g == 0:
            z_pass(0)

    ctail = big_c.shape[1] - width
    big_c[:, width:, :] = jnp.zeros((slots // half, ctail, half), F32)
    for r in range(n):
        for h in range(slots // half):
            cot_mine[r % nc, r // nc, :, h * half : (h + 1) * half] = big_c[
                h, r * shard : r * shard + rows_pad, :
            ].astype(BF)
    cot_cps = begin(exchange(cot_mine, cot_recv, cot_ss, cot_rs, dc, nc, at_c))

    for cp in loads[10:]:
        cp.wait()
    rows = vis.shape[0]
    images = counts.shape[1]
    place = lax.broadcasted_iota(jnp.int32, (1, rows), 1)
    target = jnp.full((1, rows), -1, jnp.int32)
    start = jnp.int32(0)
    for i in range(images):
        cnt, off = counts[0, i], offsets[0, i]
        before = jnp.int32(0)
        for e in range(i):
            before = before + jnp.where(offsets[0, e] == off, counts[0, e], 0)
        inside = (place >= start) & (place < start + cnt)
        target = jnp.where(inside, (off - 1) * cap + before + place - start, target)
        start = start + cnt
    slot_id = lax.broadcasted_iota(jnp.int32, (spread * cap, rows), 0)
    select = jnp.where(slot_id == target, 1.0, 0.0).astype(BF)

    def hand_copy(f, k):
        to = lax.rem(me + k, n)
        inside = lax.rem(to, nc)
        return copy_to(pack.at[f, k - 1], hbuf.at[f, inside, k - 1], h_ss.at[f, k - 1], h_rs.at[f, k - 1], {"dp": to})

    def share_copy(f, k, j):
        to = lax.rem(dc + j, nc)
        block = hbuf.at[f, dc, k - 1]
        return copy_to(block, block, g_ss.at[f, k - 1, j - 1], g_rs.at[f, k - 1, j - 1], {"dp": at_c(to)})

    def encode(f):
        z_sum(f)
        at = feat(col, f, fw)
        encoded = (vis[:, at].astype(F32) + scale[:, at] * (z_own[f] + fc2_b[:, at])).astype(BF)
        packed = jnp.dot(select, encoded, preferred_element_type=F32).astype(BF)
        for k in range(1, spread + 1):
            pack[f, k - 1] = packed[(k - 1) * cap : k * cap, :]
        for k in range(spread, 0, -1):
            hand_copy(f, k).start()

    def hand_wait(f):
        for k in range(1, spread + 1):
            hand_copy(f, k).wait_recv()
            for j in range(1, nc):
                share_copy(f, k, j).start()
        for k in range(1, spread + 1):
            for j in range(1, nc):
                share_copy(f, k, j).wait_recv()

    def product_of(f, to):
        got = hbuf[f, dc].reshape(slots, fw)
        total = jnp.dot(cot_mine[dc, to], got, preferred_element_type=F32)
        for j in range(1, nc):
            other = hbuf[f, lax.rem(dc + nc - j, nc)].reshape(slots, fw)
            total = total + jnp.dot(cot_recv[j - 1, to], other, preferred_element_type=F32)
        return total

    top = x1.shape[-2]

    def staged(f):
        for a in range(na):
            for b in range(nb):
                total = product_of(f, b * na + a).astype(BF)
                x1[f, a, b] = total[:top]
                y1[f, b, a] = total[top:]
        begin(x_first(f, True) + y_first(f, True))
        begin(x_first(f, False) + y_first(f, False))

    def first_stage(buf, got, ss, rs, digit, q, other, q2, peer_of, far):
        cps = []
        for j in range(1, q):
            to = lax.rem(digit + j, q)
            for i in range(1, q2) if far else (0,):
                at = lax.rem(other + i, q2)
                cps.append(
                    copy_to(buf.at[to, at], got.at[j - 1, at], ss.at[j - 1, i], rs.at[j - 1, i], {"dp": peer_of(to)})
                )
        return cps

    def x_first(f, far):
        return first_stage(x1.at[f], x1r.at[f], x1_s.at[f], x1_r.at[f], da, na, db, nb, at_a, far)

    def y_first(f, far):
        return first_stage(y1.at[f], y1r.at[f], y1_s.at[f], y1_r.at[f], db, nb, da, na, at_b, far)

    def x_second(f):
        return exchange(x2.at[f], x2r.at[f], x2_s.at[f], x2_r.at[f], db, nb, at_b)

    def y_second(f):
        return exchange(y2.at[f], y2r.at[f], y2_s.at[f], y2_r.at[f], da, na, at_a)

    def staged_next(f):
        for cp in x_first(f, True):
            cp.wait_recv()
        for j in range(1, nb):
            b = lax.rem(db + j, nb)
            x2[f, b] = added(x1.at[f], x1r.at[f], da, na, (b,)).astype(BF)
        begin(x_second(f))
        for cp in y_first(f, True):
            cp.wait_recv()
        for j in range(1, na):
            a = lax.rem(da + j, na)
            y2[f, a] = added(y1.at[f], y1r.at[f], db, nb, (a,)).astype(BF)
        begin(y_second(f))

    for f in range(1, nf):
        z_pass(f)
    s2k = exchange(k2, k2r, k2_s, k2_r, db, nb, at_b)
    s2v = exchange(v2, v2r, v2_s, v2_r, da, na, at_a)

    def key_third():
        for g in range(groups):
            for j in range(1, na):
                k1_copy(j, g).wait_recv()
        for b in range(nb):
            k2[b] = added(k1, k1r, da, na, (b,)).astype(BF)
        begin(s2k)

    def value_third():
        for j in range(1, nb):
            v1_copy(j).wait_recv()
        for a in range(na):
            v2[a] = added(v1, v1r, db, nb, (a,)).astype(BF)
        begin(s2v)

    encode(0)
    key_third()
    for f in range(1, nf):
        encode(f)
    value_third()
    for cp in cot_cps:
        cp.wait_recv()
    for f in range(nf):
        hand_wait(f)
        staged(f)
    for f in range(nf):
        staged_next(f)

    for f in range(nf):
        hand_o[:, f * fw : (f + 1) * fw] = hbuf[f, dc].reshape(slots, fw)
    for cp in s2k:
        cp.wait_recv()
    key_o[...] = added(k2, k2r, db, nb, ())[:shard]
    for cp in s2v:
        cp.wait_recv()
    val_o[...] = added(v2, v2r, da, na, ())[:shard]
    for f in range(nf):
        z_drain(f)
        for k in range(1, spread + 1):
            hand_copy(f, k).wait_send()
            for j in range(1, nc):
                share_copy(f, k, j).wait_send()
    for g in range(groups):
        for cp in kv_first(k0, k0r, k0_s, k0_r, g) + kv_first(v0, v0r, v0_s, v0_r, g):
            cp.wait_send()
        for j in range(1, na):
            k1_copy(j, g).wait_send()
    for j in range(1, nb):
        v1_copy(j).wait_send()
    for cp in cot_cps + s2k + s2v:
        cp.wait_send()
    for f in range(nf):
        for cp in x_first(f, True) + y_first(f, True) + x_first(f, False) + y_first(f, False):
            cp.wait_send()

    def kept(buf, first, second, digit, q, other, q2):
        total = buf[digit, other].astype(F32)
        for j in range(1, q):
            total = total + first[j - 1, other].astype(F32)
        for j in range(1, q2):
            total = total + second[j - 1].astype(F32)
        return total

    for f in range(nf):
        at = slice(f * fw, (f + 1) * fw)
        for cp in x_first(f, False) + y_first(f, False):
            cp.wait_recv()
        for cp in x_second(f):
            cp.wait_recv()
        proj_o[:top, at] = kept(x1.at[f], x1r.at[f], x2r.at[f], da, na, db, nb)
        for cp in y_second(f):
            cp.wait_recv()
        proj_o[top:, at] = kept(y1.at[f], y1r.at[f], y2r.at[f], db, nb, da, na)[: shard - top]
    for f in range(nf):
        for cp in x_second(f) + y_second(f):
            cp.wait_send()


def finish(*refs):
    half = len(refs) // 2
    sems = refs[-1]
    cps = []
    for i, (src, dst) in enumerate(zip(refs[:half], refs[half:-1])):
        cp = pltpu.make_async_copy(src, dst, sems.at[i])
        cp.start()
        cps.append(cp)
    for cp in cps:
        cp.wait()


def per_device(
    n, mp, hidden_rows, key_grad, value_grad, visual_rows, visual_cotangent, norm_gain, norm_bias,
    fc1_weight, fc1_bias, fc2_weight, fc2_bias, layer_scale, token_counts, dest_offsets,
):
    tokens, width = hidden_rows.shape
    spread, cap = visual_cotangent.shape[1:3]
    slots = spread * cap
    shard = (width + n) // n
    rp = up(shard, 8)
    nc, na, nb = factors(n)
    chips = n // nc
    kc = key_grad.shape[1]
    rows, feats = visual_rows.shape
    fcol = feats // mp
    nf = max(1, fcol // 128)
    fw = fcol // nf
    groups = 2 if nb % 2 == 0 else 1
    tall = up(max((n - 1) * shard + rp, width + 8), 8)
    top = up(rp // 2, 8)
    low = max(rp - top, 8)
    ns = nf
    any_spec = pl.BlockSpec(memory_space=pl.ANY)
    vm = pl.BlockSpec(memory_space=pltpu.VMEM)
    dma = lambda *s: pltpu.SemaphoreType.DMA(tuple(max(x, 1) for x in s))
    bf = lambda *s: pltpu.VMEM(tuple(max(x, 1) for x in s), BF)

    def stages(q1, q2):
        return [
            bf(nc, nb, na, rp, kc), bf(nc - 1, nb, na, rp, kc),
            bf(q1, q2, rp, kc), bf(q1 - 1, q2, rp, kc),
            bf(q2, rp, kc), bf(q2 - 1, rp, kc),
        ]

    def halves(q1, q2, h):
        return [bf(ns, q1, q2, h, fw), bf(ns, q1 - 1, q2, h, fw), bf(ns, q2, h, fw), bf(ns, q2 - 1, h, fw)]

    small = (norm_gain, norm_bias, fc1_bias, fc2_bias, layer_scale)
    outs = pl.pallas_call(
        functools.partial(kernel, (n, mp, shard, rp, spread, cap, nf, groups)),
        out_shape=(
            pltpu.VMEM((shard, kc), F32),
            pltpu.VMEM((shard, kc), F32),
            pltpu.VMEM((shard, fcol), F32),
            pltpu.VMEM((slots, fcol), BF),
        ),
        in_specs=[any_spec] * 14,
        out_specs=(vm, vm, vm, vm),
        scratch_shapes=[
            pltpu.VMEM(x.shape, BF)
            for x in (hidden_rows, key_grad, value_grad, visual_rows)
        ]
        + [bf(slots, width), bf(*fc1_weight.shape), bf(*fc2_weight.shape)]
        + [pltpu.VMEM((1, x.shape[0]), F32) for x in small]
        + [pltpu.SMEM(token_counts.shape, jnp.int32), pltpu.SMEM(dest_offsets.shape, jnp.int32)]
        + [
            pltpu.VMEM((tall, kc), F32),
            pltpu.VMEM((tall, kc), F32),
            pltpu.VMEM((slots // 128, tall, 128), F32),
            bf(nc, chips, rp, slots),
            bf(nc - 1, chips, rp, slots),
        ]
        + stages(na, nb)
        + stages(nb, na)
        + [
            pltpu.VMEM((nf, mp, rows, fw), F32),
            pltpu.VMEM((nf, rows, fw), F32),
            bf(nf, mp, rows, fw),
            bf(nf, mp - 1, rows, fw),
            bf(nf, rows, fw),
            bf(nf, spread, cap, fw),
            bf(nf, nc, spread, cap, fw),
        ]
        + halves(na, nb, top)
        + halves(nb, na, low)
        + [dma(14), dma(nc - 1), dma(nc - 1), dma(nf, mp - 1), dma(nf, mp - 1), dma(nf), dma(nf)]
        + [dma(nc - 1, groups), dma(nc - 1, groups), dma(na - 1, groups), dma(na - 1, groups), dma(nb - 1), dma(nb - 1)]
        + [dma(nc - 1, groups), dma(nc - 1, groups), dma(nb - 1), dma(nb - 1), dma(na - 1), dma(na - 1)]
        + [dma(nf, spread), dma(nf, spread), dma(nf, spread, nc - 1), dma(nf, spread, nc - 1)]
        + [dma(ns, na - 1, nb), dma(ns, na - 1, nb), dma(ns, nb - 1), dma(ns, nb - 1)]
        + [dma(ns, nb - 1, na), dma(ns, nb - 1, na), dma(ns, na - 1), dma(ns, na - 1)],
        compiler_params=pltpu.CompilerParams(
            collective_id=0, has_side_effects=True, vmem_limit_bytes=56 * 1024 * 1024
        ),
    )(
        hidden_rows, key_grad, value_grad, visual_rows, visual_cotangent.reshape(slots, width),
        fc1_weight, fc2_weight, *(x[None] for x in small), token_counts, dest_offsets,
    )
    outs = pl.pallas_call(
        finish,
        out_shape=tuple(jax.ShapeDtypeStruct(x.shape, x.dtype) for x in outs),
        in_specs=[vm] * 4,
        out_specs=(any_spec,) * 4,
        scratch_shapes=[dma(4)],
    )(*(pltpu.with_memory_space_constraint(x, pltpu.VMEM) for x in outs))
    return outs[0], outs[1], outs[2], outs[3].reshape(1, spread, cap, fcol)


def solution(mesh):
    placed = (
        P("dp", None), P("dp", "mp"), P("dp", "mp"), P("dp", None), P("dp", None, None, None),
        P(), P(), P(None, "mp"), P("mp"), P("mp", None), P(), P(), P("dp", None), P("dp", None),
    )
    return jax.shard_map(
        functools.partial(per_device, mesh.shape["dp"], mesh.shape["mp"]),
        mesh=mesh,
        in_specs=placed,
        out_specs=(P("dp", "mp"), P("dp", "mp"), P("dp", "mp"), P("dp", None, None, "mp")),
        check_vma=False,
    )
```

```python
import functools

import jax
import jax.numpy as jnp
from jax import lax
from jax.experimental import pallas as pl
from jax.experimental.pallas import tpu as pltpu
from jax.sharding import PartitionSpec as P

MESH = pl.DeviceIdType.MESH
BF = jnp.bfloat16
F32 = jnp.float32


def up(x, m):
    return -(-x // m) * m


def factors(n):
    core = 2 if n % 2 == 0 else 1
    rest = n // core
    inner = max(f for f in range(1, rest + 1) if rest % f == 0 and f * f <= rest)
    return core, inner, rest // inner


def erf_gelu(x):
    return 0.5 * x * (1.0 + lax.erf(x * (0.5**0.5)))


def kernel(
    cfg,
    hid_h, key_h, val_h, vis_h, cot_h, fc1_h, fc2_h,
    gain_h, beta_h, fc1_bh, fc2_bh, scale_h, counts_h, offsets_h,
    key_o, val_o, proj_o, hand_o,
    hid, key, val, vis, cot, fc1, fc2,
    gain, beta, fc1_b, fc2_b, scale, counts, offsets,
    big_k, big_v, big_c,
    cot_mine, cot_recv,
    k0, k0r, k1, k1r, k2, k2r,
    v0, v0r, v1, v1r, v2, v2r,
    z_full, z_own, z_send, z_recv, z_relay, pack, hbuf,
    x1, x1r, x2, x2r, y1, y1r, y2, y2r,
    load_sem, cot_ss, cot_rs, z_ss, z_rs, e_ss, e_rs,
    k0_s, k0_r, k1_s, k1_r, k2_s, k2_r,
    v0_s, v0_r, v1_s, v1_r, v2_s, v2_r,
    h_ss, h_rs, g_ss, g_rs,
    x1_s, x1_r, x2_s, x2_r, y1_s, y1_r, y2_s, y2_r,
):
    n, mp, shard, rows_pad, spread, cap, nf, groups = cfg
    nc, na, nb = factors(n)
    chips = n // nc
    me = lax.axis_index("dp")
    col = lax.axis_index("mp")
    dc = lax.rem(me, nc)
    da = lax.rem(lax.div(me, nc), na)
    db = lax.div(me, nc * na)
    chip = lax.div(me, nc)
    tokens, width = hid.shape
    slots = cot.shape[0]
    kc = key.shape[1]
    fcol = hand_o.shape[1]
    fw = fcol // nf

    def rank(c, a, b):
        return (b * na + a) * nc + c

    loads = []
    for i, (src, dst) in enumerate(
        (
            (vis_h, vis), (gain_h, gain), (beta_h, beta), (fc1_h, fc1), (fc1_bh, fc1_b), (fc2_h, fc2),
            (key_h, key), (val_h, val), (hid_h, hid), (cot_h, cot),
            (fc2_bh, fc2_b), (scale_h, scale), (counts_h, counts), (offsets_h, offsets),
        )
    ):
        cp = pltpu.make_async_copy(src, dst, load_sem.at[i])
        cp.start()
        loads.append(cp)
    barrier = pltpu.get_barrier_semaphore()
    for j in range(1, n):
        pl.semaphore_signal(barrier, inc=1, device_id={"dp": lax.rem(me + j, n)}, device_id_type=MESH)
    for j in range(1, mp):
        pl.semaphore_signal(barrier, inc=1, device_id={"mp": lax.rem(col + j, mp)}, device_id_type=MESH)

    def copy_to(src, dst, ss, rs, where):
        return pltpu.make_async_remote_copy(
            src_ref=src, dst_ref=dst, send_sem=ss, recv_sem=rs, device_id=where, device_id_type=MESH
        )

    def remote(src, dst, ss, rs, where):
        cp = copy_to(src, dst, ss, rs, where)
        cp.start()
        return cp

    loads[0].wait()
    values = vis[...].astype(F32)
    center = jnp.mean(values, axis=1, keepdims=True)
    cen = values - center
    var = jnp.mean(cen * cen, axis=1, keepdims=True)
    for cp in loads[1:3]:
        cp.wait()
    normed = (cen * lax.rsqrt(var + 1e-06) * gain[...] + beta[...]).astype(BF)
    for cp in loads[3:5]:
        cp.wait()
    hidden = erf_gelu(jnp.dot(normed, fc1[...], preferred_element_type=F32) + fc1_b[...]).astype(BF)
    loads[5].wait()
    partial = jnp.dot(hidden, fc2[...], preferred_element_type=F32)
    for m in range(mp):
        for f in range(nf):
            piece = partial[:, m * fcol + f * fw : m * fcol + (f + 1) * fw]
            z_full[f, m] = piece
            z_send[f, m] = piece.astype(BF)

    def feat(i, f=0, w=fcol):
        return pl.ds(pl.multiple_of(i * fcol + f * fw, 128 if fw % 128 == 0 else fw), w)

    chain = mp >= 4
    low, high = col == 0, col == mp - 1
    if chain:
        edge = low | high
        near = jnp.where(low, 1, mp - 2)
        inner = (col == 1) | (col == mp - 2)
        beyond = jnp.where(col == 1, mp - 1, 0)
        opposite = jnp.where(low, mp - 1, 0)
    order = sorted(range(1, mp), key=lambda j: abs(j - mp / 2))

    def z_copy(f, j):
        to = lax.rem(col + j, mp)
        return copy_to(z_send.at[f, to], z_recv.at[f, j - 1], z_ss.at[f, j - 1], z_rs.at[f, j - 1], {"mp": to})

    def e_copy(f):
        return copy_to(z_send.at[f, opposite], z_relay.at[f], e_ss.at[f], e_rs.at[f], {"mp": near})

    def r_copy(f):
        j = jnp.where(col == 1, mp - 2, 2)
        return copy_to(z_send.at[f, beyond], z_recv.at[f, j - 1], z_ss.at[f, j - 1], z_rs.at[f, j - 1], {"mp": beyond})

    def held(j):
        to = lax.rem(col + j, mp)
        return (low & (to == mp - 1)) | (high & (to == 0)), ((col == 1) & (to == mp - 1)) | ((col == mp - 2) & (to == 0))

    def z_start(f):
        for j in order:
            if chain:
                skip, later = held(j)

                @pl.when(jnp.logical_not(skip | later))
                def _():
                    z_copy(f, j).start()
            else:
                z_copy(f, j).start()

    def z_pass(f):
        if chain:
            @pl.when(inner)
            def _():
                e_copy(f).wait_recv()
                z_send[f, beyond] = (z_full[f, beyond] + z_relay[f].astype(F32)).astype(BF)
                r_copy(f).start()

    def z_sum(f):
        z_own[f] = z_full[f, col]
        for j in order:
            def take():
                z_copy(f, j).wait_recv()
                z_own[f] += z_recv[f, j - 1].astype(F32)

            source = lax.rem(col + mp - j, mp)
            if chain:
                @pl.when(jnp.logical_not((low & (source == mp - 1)) | (high & (source == 0))))
                def _():
                    take()
            else:
                take()

    def z_drain(f):
        if chain:
            @pl.when(edge)
            def _():
                e_copy(f).wait_send()
        for j in order:
            if chain:
                skip, _ = held(j)

                @pl.when(jnp.logical_not(skip))
                def _():
                    z_copy(f, j).wait_send()
            else:
                z_copy(f, j).wait_send()

    pl.semaphore_wait(barrier, n - 1 + mp - 1)
    if chain:
        @pl.when(edge)
        def _():
            for f in range(nf):
                e_copy(f).start()
    for f in range(nf):
        z_start(f)

    for cp in loads[6:9]:
        cp.wait()
    kv = jnp.concatenate([key[...], val[...]], axis=1)
    tail = big_k.shape[0] - width
    first = lax.broadcasted_iota(jnp.int32, (tail, kc), 0) == 0
    big_k[width:, :] = jnp.where(first, jnp.sum(key[...].astype(F32), axis=0, keepdims=True), 0.0)
    big_v[width:, :] = jnp.where(first, jnp.sum(val[...].astype(F32), axis=0, keepdims=True), 0.0)
    nbg = nb // groups
    at_c = lambda c: rank(c, da, db)
    at_a = lambda a: rank(dc, a, db)
    at_b = lambda b: rank(dc, da, b)

    def kv_first(buf, got, ss, rs, g):
        part = pl.ds(g * nbg, nbg)
        cps = []
        for j in range(1, nc):
            to = lax.rem(dc + j, nc)
            cps.append(copy_to(buf.at[to, part], got.at[j - 1, part], ss.at[j - 1, g], rs.at[j - 1, g], {"dp": at_c(to)}))
        return cps

    block = width if groups == 1 else min(width, up((nbg * na * nc - 1) * shard + rows_pad, 128))
    stride = 0 if groups == 1 else (width - block) // (groups - 1)

    def product(i, _):
        at = pl.multiple_of(i * stride, 128)
        res = lax.dot_general(
            hid[:, pl.ds(at, block)], kv, (((0,), (0,)), ((), ())), preferred_element_type=F32
        )
        big_k[pl.ds(at, block), :] = res[:, :kc]
        big_v[pl.ds(at, block), :] = res[:, kc:]
        for g in range(groups):
            @pl.when(i == g)
            def _():
                for b in range(g * nbg, (g + 1) * nbg):
                    for a in range(na):
                        for c in range(nc):
                            r = rank(c, a, b)
                            k0[c, b, a] = big_k[r * shard : r * shard + rows_pad, :].astype(BF)
                            v0[c, b, a] = big_v[r * shard : r * shard + rows_pad, :].astype(BF)
                for cp in kv_first(k0, k0r, k0_s, k0_r, g) + kv_first(v0, v0r, v0_s, v0_r, g):
                    cp.start()
        return 0

    lax.fori_loop(0, groups, product, 0)

    def exchange(buf, got, ss, rs, digit, q, peer_of):
        cps = []
        for j in range(1, q):
            to = lax.rem(digit + j, q)
            cps.append(copy_to(buf.at[to], got.at[j - 1], ss.at[j - 1], rs.at[j - 1], {"dp": peer_of(to)}))
        return cps

    def begin(cps):
        for cp in cps:
            cp.start()
        return cps

    def added(buf, got, digit, q, at):
        total = buf[(digit,) + at].astype(F32)
        for j in range(1, q):
            total = total + got[(j - 1,) + at].astype(F32)
        return total

    loads[9].wait()
    half = 128
    step = width // 2 if width % 256 == 0 else 128

    def turn(i, _):
        at = pl.multiple_of(i * step, 128)
        for h in range(slots // half):
            piece = cot[h * half : (h + 1) * half, pl.ds(at, step)].astype(F32)
            big_c[h, pl.ds(at, step), :] = piece.T
        return 0

    lax.fori_loop(0, width // step, turn, 0)

    def kv_second(g):
        for b in range(g * nbg, (g + 1) * nbg):
            for a in range(na):
                k1[a, b] = added(k0, k0r, dc, nc, (b, a)).astype(BF)
                v1[b, a] = added(v0, v0r, dc, nc, (b, a)).astype(BF)
        part = pl.ds(g * nbg, nbg)
        for j in range(1, na):
            k1_copy(j, g).start()
        for j in range(1, nb):
            @pl.when(lax.div(lax.rem(db + j, nb), nbg) == g)
            def _():
                v1_copy(j).start()

    def k1_copy(j, g):
        part = pl.ds(g * nbg, nbg)
        to = lax.rem(da + j, na)
        return copy_to(k1.at[to, part], k1r.at[j - 1, part], k1_s.at[j - 1, g], k1_r.at[j - 1, g], {"dp": at_a(to)})

    def v1_copy(j):
        to = lax.rem(db + j, nb)
        return copy_to(v1.at[to], v1r.at[j - 1], v1_s.at[j - 1], v1_r.at[j - 1], {"dp": at_b(to)})

    for g in range(groups):
        for cp in kv_first(k0, k0r, k0_s, k0_r, g) + kv_first(v0, v0r, v0_s, v0_r, g):
            cp.wait_recv()
        kv_second(g)
        if g == 0:
            z_pass(0)

    ctail = big_c.shape[1] - width
    big_c[:, width:, :] = jnp.zeros((slots // half, ctail, half), F32)
    for r in range(n):
        for h in range(slots // half):
            cot_mine[r % nc, r // nc, :, h * half : (h + 1) * half] = big_c[
                h, r * shard : r * shard + rows_pad, :
            ].astype(BF)
    cot_cps = begin(exchange(cot_mine, cot_recv, cot_ss, cot_rs, dc, nc, at_c))

    for cp in loads[10:]:
        cp.wait()
    rows = vis.shape[0]
    images = counts.shape[1]
    place = lax.broadcasted_iota(jnp.int32, (1, rows), 1)
    target = jnp.full((1, rows), -1, jnp.int32)
    start = jnp.int32(0)
    for i in range(images):
        cnt, off = counts[0, i], offsets[0, i]
        before = jnp.int32(0)
        for e in range(i):
            before = before + jnp.where(offsets[0, e] == off, counts[0, e], 0)
        inside = (place >= start) & (place < start + cnt)
        target = jnp.where(inside, (off - 1) * cap + before + place - start, target)
        start = start + cnt
    slot_id = lax.broadcasted_iota(jnp.int32, (spread * cap, rows), 0)
    select = jnp.where(slot_id == target, 1.0, 0.0).astype(BF)

    def hand_copy(f, k):
        to = lax.rem(me + k, n)
        inside = lax.rem(to, nc)
        return copy_to(pack.at[f, k - 1], hbuf.at[f, inside, k - 1], h_ss.at[f], h_rs.at[f], {"dp": to})

    def hand_all(f):
        return copy_to(pack.at[f], hbuf.at[f, dc], h_ss.at[f], h_rs.at[f], {"dp": lax.rem(me + 1, n)})

    def share_copy(f, j):
        to = lax.rem(dc + j, nc)
        block = hbuf.at[f, dc]
        return copy_to(block, block, g_ss.at[f, j - 1], g_rs.at[f, j - 1], {"dp": at_c(to)})

    def encode(f):
        z_sum(f)
        at = feat(col, f, fw)
        encoded = (vis[:, at].astype(F32) + scale[:, at] * (z_own[f] + fc2_b[:, at])).astype(BF)
        packed = jnp.dot(select, encoded, preferred_element_type=F32).astype(BF)
        for k in range(1, spread + 1):
            pack[f, k - 1] = packed[(k - 1) * cap : k * cap, :]
        for k in range(spread, 0, -1):
            hand_copy(f, k).start()

    def hand_wait(f):
        hand_all(f).wait_recv()
        for j in range(1, nc):
            share_copy(f, j).start()
        for j in range(1, nc):
            share_copy(f, j).wait_recv()

    def product_of(f, to):
        got = hbuf[f, dc].reshape(slots, fw)
        total = jnp.dot(cot_mine[dc, to], got, preferred_element_type=F32)
        for j in range(1, nc):
            other = hbuf[f, lax.rem(dc + nc - j, nc)].reshape(slots, fw)
            total = total + jnp.dot(cot_recv[j - 1, to], other, preferred_element_type=F32)
        return total

    top = x1.shape[-2]

    def staged(f):
        def fill(pairs):
            for ja, jb in pairs:
                a, b = lax.rem(da + ja, na), lax.rem(db + jb, nb)
                total = product_of(f, b * na + a).astype(BF)
                x1[f, a, b] = total[:top]
                y1[f, b, a] = total[top:]

        pairs = [(ja, jb) for ja in range(na) for jb in range(nb)]
        fill([p for p in pairs if p[0] and p[1]])
        begin(x_first(f, True) + y_first(f, True))
        fill([p for p in pairs if not (p[0] and p[1])])
        begin(x_first(f, False) + y_first(f, False))

    def first_stage(buf, got, ss, rs, digit, q, other, q2, peer_of, far):
        cps = []
        for j in range(1, q):
            to = lax.rem(digit + j, q)
            for i in range(1, q2) if far else (0,):
                at = lax.rem(other + i, q2)
                cps.append(
                    copy_to(buf.at[to, at], got.at[j - 1, at], ss.at[j - 1, i], rs.at[j - 1, i], {"dp": peer_of(to)})
                )
        return cps

    def x_first(f, far):
        return first_stage(x1.at[f], x1r.at[f], x1_s.at[f], x1_r.at[f], da, na, db, nb, at_a, far)

    def y_first(f, far):
        return first_stage(y1.at[f], y1r.at[f], y1_s.at[f], y1_r.at[f], db, nb, da, na, at_b, far)

    def x_second(f):
        return exchange(x2.at[f], x2r.at[f], x2_s.at[f], x2_r.at[f], db, nb, at_b)

    def y_second(f):
        return exchange(y2.at[f], y2r.at[f], y2_s.at[f], y2_r.at[f], da, na, at_a)

    def staged_next(f):
        for cp in x_first(f, True):
            cp.wait_recv()
        for j in range(1, nb):
            b = lax.rem(db + j, nb)
            x2[f, b] = added(x1.at[f], x1r.at[f], da, na, (b,)).astype(BF)
        begin(x_second(f))
        for cp in y_first(f, True):
            cp.wait_recv()
        for j in range(1, na):
            a = lax.rem(da + j, na)
            y2[f, a] = added(y1.at[f], y1r.at[f], db, nb, (a,)).astype(BF)
        begin(y_second(f))

    for f in range(1, nf):
        z_pass(f)
    s2k = exchange(k2, k2r, k2_s, k2_r, db, nb, at_b)
    s2v = exchange(v2, v2r, v2_s, v2_r, da, na, at_a)

    def key_third():
        for g in range(groups):
            for j in range(1, na):
                k1_copy(j, g).wait_recv()
        for b in range(nb):
            k2[b] = added(k1, k1r, da, na, (b,)).astype(BF)
        begin(s2k)

    def value_third():
        for j in range(1, nb):
            v1_copy(j).wait_recv()
        for a in range(na):
            v2[a] = added(v1, v1r, db, nb, (a,)).astype(BF)
        begin(s2v)

    encode(0)
    key_third()
    for f in range(1, nf):
        encode(f)
    value_third()
    for cp in cot_cps:
        cp.wait_recv()
    for f in range(nf):
        hand_wait(f)
        staged(f)
    for f in range(nf):
        staged_next(f)

    for f in range(nf):
        hand_o[:, f * fw : (f + 1) * fw] = hbuf[f, dc].reshape(slots, fw)
    for cp in s2k:
        cp.wait_recv()
    key_o[...] = added(k2, k2r, db, nb, ())[:shard]
    for cp in s2v:
        cp.wait_recv()
    val_o[...] = added(v2, v2r, da, na, ())[:shard]
    for f in range(nf):
        z_drain(f)
        hand_all(f).wait_send()
        for j in range(1, nc):
            share_copy(f, j).wait_send()
    for g in range(groups):
        for cp in kv_first(k0, k0r, k0_s, k0_r, g) + kv_first(v0, v0r, v0_s, v0_r, g):
            cp.wait_send()
        for j in range(1, na):
            k1_copy(j, g).wait_send()
    for j in range(1, nb):
        v1_copy(j).wait_send()
    for cp in cot_cps + s2k + s2v:
        cp.wait_send()
    for f in range(nf):
        for cp in x_first(f, True) + y_first(f, True) + x_first(f, False) + y_first(f, False):
            cp.wait_send()

    def kept(buf, first, second, digit, q, other, q2):
        total = buf[digit, other].astype(F32)
        for j in range(1, q):
            total = total + first[j - 1, other].astype(F32)
        for j in range(1, q2):
            total = total + second[j - 1].astype(F32)
        return total

    for f in range(nf):
        at = slice(f * fw, (f + 1) * fw)
        for cp in x_first(f, False) + y_first(f, False):
            cp.wait_recv()
        for cp in x_second(f):
            cp.wait_recv()
        proj_o[:top, at] = kept(x1.at[f], x1r.at[f], x2r.at[f], da, na, db, nb)
        for cp in y_second(f):
            cp.wait_recv()
        proj_o[top:, at] = kept(y1.at[f], y1r.at[f], y2r.at[f], db, nb, da, na)[: shard - top]
    for f in range(nf):
        for cp in x_second(f) + y_second(f):
            cp.wait_send()


def finish(*refs):
    half = len(refs) // 2
    sems = refs[-1]
    cps = []
    for i, (src, dst) in enumerate(zip(refs[:half], refs[half:-1])):
        cp = pltpu.make_async_copy(src, dst, sems.at[i])
        cp.start()
        cps.append(cp)
    for cp in cps:
        cp.wait()


def per_device(
    n, mp, hidden_rows, key_grad, value_grad, visual_rows, visual_cotangent, norm_gain, norm_bias,
    fc1_weight, fc1_bias, fc2_weight, fc2_bias, layer_scale, token_counts, dest_offsets,
):
    tokens, width = hidden_rows.shape
    spread, cap = visual_cotangent.shape[1:3]
    slots = spread * cap
    shard = (width + n) // n
    rp = up(shard, 8)
    nc, na, nb = factors(n)
    chips = n // nc
    kc = key_grad.shape[1]
    rows, feats = visual_rows.shape
    fcol = feats // mp
    nf = max(1, fcol // 128)
    fw = fcol // nf
    groups = 2 if nb % 2 == 0 else 1
    tall = up(max((n - 1) * shard + rp, width + 8), 8)
    top = up(rp // 2, 8)
    low = max(rp - top, 8)
    ns = nf
    any_spec = pl.BlockSpec(memory_space=pl.ANY)
    vm = pl.BlockSpec(memory_space=pltpu.VMEM)
    dma = lambda *s: pltpu.SemaphoreType.DMA(tuple(max(x, 1) for x in s))
    bf = lambda *s: pltpu.VMEM(tuple(max(x, 1) for x in s), BF)

    def stages(q1, q2):
        return [
            bf(nc, nb, na, rp, kc), bf(nc - 1, nb, na, rp, kc),
            bf(q1, q2, rp, kc), bf(q1 - 1, q2, rp, kc),
            bf(q2, rp, kc), bf(q2 - 1, rp, kc),
        ]

    def halves(q1, q2, h):
        return [bf(ns, q1, q2, h, fw), bf(ns, q1 - 1, q2, h, fw), bf(ns, q2, h, fw), bf(ns, q2 - 1, h, fw)]

    small = (norm_gain, norm_bias, fc1_bias, fc2_bias, layer_scale)
    outs = pl.pallas_call(
        functools.partial(kernel, (n, mp, shard, rp, spread, cap, nf, groups)),
        out_shape=(
            pltpu.VMEM((shard, kc), F32),
            pltpu.VMEM((shard, kc), F32),
            pltpu.VMEM((shard, fcol), F32),
            pltpu.VMEM((slots, fcol), BF),
        ),
        in_specs=[any_spec] * 14,
        out_specs=(vm, vm, vm, vm),
        scratch_shapes=[
            pltpu.VMEM(x.shape, BF)
            for x in (hidden_rows, key_grad, value_grad, visual_rows)
        ]
        + [bf(slots, width), bf(*fc1_weight.shape), bf(*fc2_weight.shape)]
        + [pltpu.VMEM((1, x.shape[0]), F32) for x in small]
        + [pltpu.SMEM(token_counts.shape, jnp.int32), pltpu.SMEM(dest_offsets.shape, jnp.int32)]
        + [
            pltpu.VMEM((tall, kc), F32),
            pltpu.VMEM((tall, kc), F32),
            pltpu.VMEM((slots // 128, tall, 128), F32),
            bf(nc, chips, rp, slots),
            bf(nc - 1, chips, rp, slots),
        ]
        + stages(na, nb)
        + stages(nb, na)
        + [
            pltpu.VMEM((nf, mp, rows, fw), F32),
            pltpu.VMEM((nf, rows, fw), F32),
            bf(nf, mp, rows, fw),
            bf(nf, mp - 1, rows, fw),
            bf(nf, rows, fw),
            bf(nf, spread, cap, fw),
            bf(nf, nc, spread, cap, fw),
        ]
        + halves(na, nb, top)
        + halves(nb, na, low)
        + [dma(14), dma(nc - 1), dma(nc - 1), dma(nf, mp - 1), dma(nf, mp - 1), dma(nf), dma(nf)]
        + [dma(nc - 1, groups), dma(nc - 1, groups), dma(na - 1, groups), dma(na - 1, groups), dma(nb - 1), dma(nb - 1)]
        + [dma(nc - 1, groups), dma(nc - 1, groups), dma(nb - 1), dma(nb - 1), dma(na - 1), dma(na - 1)]
        + [dma(nf), dma(nf), dma(nf, nc - 1), dma(nf, nc - 1)]
        + [dma(ns, na - 1, nb), dma(ns, na - 1, nb), dma(ns, nb - 1), dma(ns, nb - 1)]
        + [dma(ns, nb - 1, na), dma(ns, nb - 1, na), dma(ns, na - 1), dma(ns, na - 1)],
        compiler_params=pltpu.CompilerParams(
            collective_id=0, has_side_effects=True, vmem_limit_bytes=56 * 1024 * 1024
        ),
    )(
        hidden_rows, key_grad, value_grad, visual_rows, visual_cotangent.reshape(slots, width),
        fc1_weight, fc2_weight, *(x[None] for x in small), token_counts, dest_offsets,
    )
    outs = pl.pallas_call(
        finish,
        out_shape=tuple(jax.ShapeDtypeStruct(x.shape, x.dtype) for x in outs),
        in_specs=[vm] * 4,
        out_specs=(any_spec,) * 4,
        scratch_shapes=[dma(4)],
    )(*(pltpu.with_memory_space_constraint(x, pltpu.VMEM) for x in outs))
    return outs[0], outs[1], outs[2], outs[3].reshape(1, spread, cap, fcol)


def solution(mesh):
    placed = (
        P("dp", None), P("dp", "mp"), P("dp", "mp"), P("dp", None), P("dp", None, None, None),
        P(), P(), P(None, "mp"), P("mp"), P("mp", None), P(), P(), P("dp", None), P("dp", None),
    )
    return jax.shard_map(
        functools.partial(per_device, mesh.shape["dp"], mesh.shape["mp"]),
        mesh=mesh,
        in_specs=placed,
        out_specs=(P("dp", "mp"), P("dp", "mp"), P("dp", "mp"), P("dp", None, None, "mp")),
        check_vma=False,
    )
```
